32 devices in a mesh: data: 2 (over x), hid: 4 (over z), vocab: 4 (over y, core).
Axes of the slice: x: 2, y: 2, z: 4, core: 2. Of those that a mesh axis runs over, the one named last changes fastest.
Arguments:
- h_states: bfloat16 [64, 1152], P('data', 'hid'), parts along dimension 0
- w_head: bfloat16 [1152, 262144], P('hid', 'vocab')
- inv_temp: float32 [64], P('data'), parts along dimension 0
- tgt_ids: int32 [64], P('data'), parts along dimension 0
Outputs:
- output 1: float32 [64, 262144], P('data', ('vocab', 'hid')), parts along dimension 0
- output 2: float32 [64], P('data'), parts along dimension 0
There are 2 independent parts. The reference program is written for one: setup_inputs(seed, part) draws one part's arguments, and reference() takes and returns one part's arrays. A program takes and returns all parts, laid end to end along the dimension named above; an argument that names none is the same for every part.
All inputs are finite; a program needn't handle non-finite values.
Results may differ from the reference program's by a relative error of at most 0.001.
Values are sent between devices in bfloat16 or wider.
A program may use at most 1 GiB of HBM per device.

```python
import jax
import jax.numpy as jnp
from jax import lax
import math

B = 32
D = 1152
V = 262144


def setup_inputs(seed: int = 0, part: int = 0) -> dict:
    part_keys = jax.random.split(jax.random.fold_in(jax.random.key(seed), part), 5)
    shared_keys = jax.random.split(jax.random.key(seed + 1), 2)
    common_dir = jax.random.normal(shared_keys[0], (D,), jnp.float32)
    col_level = 140.0 - 2.5 * jnp.arange(V, dtype=jnp.float32) / V
    row_keys = jax.random.split(shared_keys[1], D // 128)
    dir_blocks = common_dir.reshape(D // 128, 128)

    def weight_block(block_args):
        blk_key, dir_part = block_args
        noise_blk = jax.random.normal(blk_key, (128, V), jnp.float32)
        w_part = noise_blk * (0.6 / math.sqrt(D)) + dir_part[:, None] * (col_level[None, :] / D)
        return w_part.astype(jnp.bfloat16)

    w_head = lax.map(weight_block, (row_keys, dir_blocks)).reshape(D, V)
    row_noise = jax.random.normal(part_keys[0], (B, D), jnp.float32)
    row_shift = jax.random.uniform(part_keys[1], (B,), jnp.float32, 1.0, 2.0)
    h_states = (row_noise + row_shift[:, None] * common_dir[None, :]).astype(jnp.bfloat16)
    inv_temp = jax.random.uniform(part_keys[2], (B,), jnp.float32, 0.7, 1.3)
    first_pick = jax.random.randint(part_keys[3], (B,), 0, V)
    second_pick = jax.random.randint(part_keys[4], (B,), 0, V)
    tgt_ids = jnp.maximum(first_pick, second_pick).at[0].set(0).at[1].set(V - 1)
    return {"h_states": h_states, "w_head": w_head, "inv_temp": inv_temp, "tgt_ids": tgt_ids}


def reference(h_states, w_head, inv_temp, tgt_ids):
    logits = jnp.dot(h_states, w_head, preferred_element_type=jnp.float32) * inv_temp[:, None]
    row_max = jnp.max(logits, axis=1, keepdims=True)
    exp_vals = jnp.exp(logits - row_max)
    row_sum = jnp.sum(exp_vals, axis=1, keepdims=True)
    prob_rows = exp_vals / row_sum
    cdf_table = jnp.cumsum(prob_rows, axis=1)
    cdf_at_tgt = jnp.take_along_axis(cdf_table, tgt_ids[:, None], axis=1)[:, 0]
    return (cdf_table, cdf_at_tgt)
```

```python
import functools

import jax
import jax.numpy as jnp
from jax import lax
from jax.experimental import pallas as pl
from jax.experimental.pallas import tpu as pltpu
from jax.sharding import PartitionSpec as P

MESH = pl.DeviceIdType.MESH
NP = 16
NX = 2
RING = 4
LAG = 2
XSTEP = 2 * NP + 4
F32 = jnp.float32
BF16 = jnp.bfloat16


def iota(shape, dim):
    return lax.broadcasted_iota(jnp.int32, shape, dim)


def to_col(row):
    n = row.shape[1]
    return jnp.sum(jnp.where(iota((32, n), 0) == iota((32, n), 1), row, 0.0), axis=1, keepdims=True)


def pack_row(m, s, t):
    sub, lane = iota((32, 128), 0), iota((32, 128), 1)
    picked = jnp.where(lane == sub, m, jnp.where(lane == sub + 32, s, jnp.where(lane == sub + 64, t, 0.0)))
    return jnp.sum(picked, axis=0, keepdims=True)


def kernel(tok, h_hbm, w_hbm, temp_ref, tgt_ref, out_ref, tgt_out_ref,
           h_buf, w_buf, part, far_in, side_in, near_in, x_part, x_src, x_in, piece_m, piece_s, piece_t,
           msg_src, msg_in, stats,
           h_sem, w_sem, far_send, far_recv, side_recv, near_send, near_recv, xp_send, xp_recv, x_send, x_recv,
           msg_send, msg_recv, st_send, st_recv):
    z, v = lax.axis_index("hid"), lax.axis_index("vocab")
    outer = (z == 0) | (z == 3)
    inner = (z == 1) | (z == 2)
    far = jnp.where(z < 2, z + 1, z - 1)
    near = jnp.where(z == 1, 0, 3)
    cols = NP * tok
    last = 3 * NP - NX

    def w_load(rel, i, slot):
        owner = jnp.where(z < 2, rel, 3 - rel)
        start = pl.multiple_of(owner * cols + i * tok, tok)
        return pltpu.make_async_copy(w_hbm.at[:, pl.ds(start, tok)], w_buf.at[slot], w_sem.at[slot])

    h_copy = pltpu.make_async_copy(h_hbm, h_buf, h_sem)
    h_copy.start()
    for slot, rel in enumerate((3, 0, 2, 1)):
        w_load(rel, 0, slot).start()

    barrier = pltpu.get_barrier_semaphore()
    for dv in range(4):
        for dz in range(4):
            if dv or dz:
                pl.semaphore_signal(barrier, inc=1, device_id={"hid": lax.rem(z + dz, 4), "vocab": lax.rem(v + dv, 4)},
                                    device_id_type=MESH)

    def product(rel, i, slot):
        w_load(rel, i, slot).wait()
        part[rel * NP + i] = jnp.dot(h_buf[...], w_buf[slot], preferred_element_type=F32)

        @pl.when(i + 1 < NP)
        def _():
            w_load(rel, i + 1, slot).start()

    def products(i):
        product(0, i, 1)
        product(2, i, 2)
        product(1, i, 3)

        @pl.when(i + 1 < NP)
        def _():
            product(3, i + 1, 0)

    tri = (iota((128, 128), 0) <= iota((128, 128), 1)).astype(BF16)
    piece_m[...] = jnp.zeros_like(piece_m)
    piece_s[...] = jnp.zeros_like(piece_s)
    piece_t[...] = jnp.zeros_like(piece_t)
    temp = to_col(temp_ref[...])
    tgt_row = tgt_ref[...].astype(F32)
    tgt = to_col(tgt_row)

    def put(ref, lane, value):
        ref[...] = jnp.where(iota((32, 128), 1) == lane, value, ref[...])

    def finish(total, first, lane, store):
        logits = total * temp
        m = jnp.max(logits, axis=1, keepdims=True)
        e = jnp.exp(logits - m)
        n_blk = tok // 128
        terms = []
        for b in range(n_blk):
            blk = e[:, b * 128:(b + 1) * 128]
            hi = blk.astype(BF16)
            rest = blk - hi.astype(F32)
            mid = rest.astype(BF16)
            low = (rest - mid.astype(F32)).astype(BF16)
            terms += [hi, mid, low]
        sums = jnp.dot(jnp.concatenate(terms, axis=0), tri, preferred_element_type=F32)
        carry = jnp.zeros((32, 1), F32)
        hit = jnp.zeros((32, 128), F32)
        pos = tgt - first
        lanes = iota((32, 128), 1).astype(F32)
        for b in range(n_blk):
            s = sums[96 * b:96 * b + 96]
            c = (s[0:32] + s[32:64] + s[64:96]) + carry
            store(b, c)
            hit = hit + jnp.where(lanes == pos - float(b * 128), c, 0.0)
            carry = c[:, 127:128]
        put(piece_m, lane, m)
        put(piece_s, lane, carry)
        put(piece_t, lane, jnp.sum(hit, axis=1, keepdims=True))

    def first_token(owner, i):
        return (((v * 4 + owner) * NP + i) * tok).astype(F32)

    def scan_lanes(x):
        lane = iota((32, 128), 1)
        for shift in (1, 2, 4, 8):
            x = x + jnp.where(lane >= shift, pltpu.roll(x, shift, 1), 0.0)
        return x

    def combine(owner):
        lane = iota((32, 128), 1)
        live = lane < NP
        m_all, s_all, t_all = piece_m[...], piece_s[...], piece_t[...]
        m = jnp.max(jnp.where(live, m_all, m_all[:, 0:1]), axis=1, keepdims=True)
        scale = jnp.where(live, jnp.exp(jnp.where(live, m_all, m) - m), 0.0)
        tot = s_all * scale
        s = jnp.sum(tot, axis=1, keepdims=True)
        low = lane.astype(F32) * float(tok) + first_token(owner, 0)
        t = jnp.sum(jnp.where(low + float(tok) <= tgt, tot, jnp.where(low <= tgt, t_all * scale, 0.0)),
                    axis=1, keepdims=True)
        return pack_row(m, s, t)

    def far_copy(src, t, dst, sems):
        return pltpu.make_async_remote_copy(src_ref=src, dst_ref=dst.at[t], send_sem=far_send.at[lax.rem(t, RING)],
                                            recv_sem=sems.at[t], device_id={"hid": far}, device_id_type=MESH)

    def outer_copy(t):
        i, ph = lax.rem(t, NP), t // NP
        return far_copy(part.at[(3 - ph) * NP + i], t, far_in, far_recv)

    def inner_copy(t):
        return far_copy(far_in.at[t], t, side_in, side_recv)

    def near_copy(g):
        return pltpu.make_async_remote_copy(src_ref=side_in.at[g], dst_ref=near_in.at[g],
                                            send_sem=near_send.at[lax.rem(g, RING)], recv_sem=near_recv.at[g],
                                            device_id={"hid": near}, device_id_type=MESH)

    def x_part_copy(k):
        return pltpu.make_async_remote_copy(src_ref=side_in.at[2 * NP - NX + k], dst_ref=x_part.at[k],
                                            send_sem=xp_send.at[k], recv_sem=xp_recv.at[k],
                                            device_id={"hid": near}, device_id_type=MESH)

    def x_copy(k):
        return pltpu.make_async_remote_copy(src_ref=x_src.at[k], dst_ref=x_in.at[k], send_sem=x_send.at[k],
                                            recv_sem=x_recv.at[k], device_id={"hid": far}, device_id_type=MESH)

    msg_copy = pltpu.make_async_remote_copy(src_ref=msg_src, dst_ref=msg_in, send_sem=msg_send, recv_sem=msg_recv,
                                            device_id={"hid": far}, device_id_type=MESH)

    h_copy.wait()
    product(3, 0, 0)
    pl.semaphore_wait(barrier, 15)

    def out_store(i):
        def store(b, c):
            out_ref[:, pl.ds(pl.multiple_of(i * tok + b * 128, 128), 128)] = c
        return store

    @pl.when(outer)
    def _():
        def step(t, _):
            i = lax.rem(t, NP)

            @pl.when(t >= RING)
            def _():
                outer_copy(t - RING).wait_send()

            outer_copy(t).start()

            @pl.when(t < NP)
            def _():
                products(i)

            @pl.when((t >= NP) & (t < 2 * NP))
            def _():
                near_copy(i).wait_recv()
                finish(part[i] + near_in[i], first_token(z, i), i, out_store(i))

            @pl.when(t == XSTEP)
            def _():
                for k in range(NX):
                    def store(b, c, k=k):
                        x_src[k, :, b * 128:(b + 1) * 128] = c
                    x_part_copy(k).wait_recv()
                    finish(part[2 * NP - NX + k] + x_part[k], first_token(far, NP - NX + k), NP + k, store)
                rows = [combine(z)]
                for k in range(NX):
                    lane = NP + k
                    rows.append(pack_row(piece_m[:, lane:lane + 1], piece_s[:, lane:lane + 1],
                                         piece_t[:, lane:lane + 1]))
                sub = iota((8, 128), 0)
                tile = jnp.zeros((8, 128), F32)
                for k, row in enumerate(rows):
                    tile = jnp.where(sub == k, row, tile)
                msg_src[...] = tile

            @pl.when(t == XSTEP + 1)
            def _():
                msg_copy.start()

            return ()

        lax.fori_loop(0, last, step, ())
        for k in range(NX):
            x_copy(k).start()
        for k in range(RING):
            outer_copy(last - RING + k).wait_send()
        msg_copy.wait_send()

    @pl.when(inner)
    def _():
        def step(t, _):
            i, ph = lax.rem(t, NP), t // NP
            g = t - LAG
            far_copy(far_in.at[t], t, far_in, far_recv).wait_recv()

            @pl.when((t >= 1) & (t <= 2 * NP))
            def _():
                @pl.when(t - 1 >= RING)
                def _():
                    inner_copy(t - 1 - RING).wait_send()
                inner_copy(t - 1).start()

            @pl.when((g >= 1) & (g <= NP))
            def _():
                @pl.when(g - 1 >= RING)
                def _():
                    near_copy(g - 1 - RING).wait_send()
                near_copy(g - 1).start()

            for k in range(NX):
                @pl.when(g - 1 == 2 * NP - NX + k)
                def _(k=k):
                    x_part_copy(k).start()

            @pl.when(t < 2 * NP)
            def _():
                far_in[t] = far_in[t] + part[(3 - ph) * NP + i]

            @pl.when((g >= 0) & (g < 2 * NP))
            def _():
                far_copy(far_in.at[g], g, side_in, side_recv).wait_recv()

                @pl.when((g < NP) | (g >= 2 * NP - NX))
                def _():
                    side_in[g] = side_in[g] + part[g]

            @pl.when(t < NP)
            def _():
                products(i)

            @pl.when(t >= 2 * NP)
            def _():
                finish(part[NP + i] + side_in[NP + i] + far_in[t], first_token(z, i), i, out_store(i))

            return ()

        lax.fori_loop(0, last, step, ())
        msg_copy.wait_recv()
        msg = msg_in[...]
        for k in range(NX):
            lane = NP - NX + k
            row = msg[k + 1:k + 2]
            put(piece_m, lane, to_col(row))
            put(piece_s, lane, to_col(pltpu.roll(row, 96, 1)))
            put(piece_t, lane, to_col(pltpu.roll(row, 64, 1)))
        mine = combine(z)
        theirs = msg[0:1]
        sub, lane = iota((8, 128), 0), iota((8, 128), 1)
        tile = jnp.where(sub == 0, jnp.where(z == 1, theirs, mine),
                         jnp.where(sub == 1, jnp.where(z == 1, mine, theirs), jnp.where(lane < 32, mine, 0.0)))
        stats[2 * v + z - 1] = tile

    def st_copy(slot, dz, dv):
        return pltpu.make_async_remote_copy(src_ref=stats.at[slot], dst_ref=stats.at[slot],
                                            send_sem=st_send.at[4 * dv + dz], recv_sem=st_recv.at[slot],
                                            device_id={"hid": lax.rem(z + dz, 4), "vocab": lax.rem(v + dv, 4)},
                                            device_id_type=MESH)

    peers = [(dz, dv) for dv in range(4) for dz in range(4) if dv or dz]

    @pl.when(inner)
    def _():
        for dz, dv in peers:
            st_copy(2 * v + z - 1, dz, dv).start()
        for k in range(RING):
            inner_copy(2 * NP - RING + k).wait_send()
            near_copy(NP - RING + k).wait_send()
        for k in range(NX):
            x_part_copy(k).wait_send()

    for slot in range(8):
        @pl.when(outer | (2 * v + z - 1 != slot))
        def _(slot=slot):
            st_copy(slot, 1, 0).wait_recv()

    table = stats[...].reshape(64, 128)
    row_id = iota((64, 128), 0)
    m_row = jnp.max(table, axis=0, keepdims=True)
    scale = jnp.exp(table - m_row)
    live = (row_id & 7) < 2
    tot = jnp.where(live, pltpu.roll(table, 96, 1) * scale, 0.0)
    t_val = jnp.where(live, pltpu.roll(table, 64, 1) * scale, 0.0)
    s_row = jnp.sum(tot, axis=0, keepdims=True)
    me = v * 16 + (z // 2) * 8 + lax.rem(z, 2)
    below_row = jnp.sum(jnp.where(row_id < me, tot, 0.0), axis=0, keepdims=True)

    low = (((row_id >> 3) * 2 + (row_id & 7)) * cols).astype(F32)
    tgt_lanes = jnp.sum(jnp.where(iota((32, 128), 0) == iota((32, 128), 1), tgt, 0.0), axis=0, keepdims=True)
    at_tgt = jnp.sum(jnp.where(low + float(cols) <= tgt_lanes, tot, jnp.where(low <= tgt_lanes, t_val, 0.0)),
                     axis=0, keepdims=True)
    tgt_out_ref[...] = (at_tgt / s_row)[:, 0:32]

    m_col, s_col, below = to_col(m_row), to_col(s_row), to_col(below_row)
    alive = iota((32, 128), 1) < NP
    mult = jnp.exp(jnp.where(alive, piece_m[...], m_col) - m_col)
    totals = jnp.where(alive, piece_s[...] * mult, 0.0)
    shift = (below + (scan_lanes(totals) - totals)) / s_col
    mult = mult / s_col

    def spread(i, src):
        out_ref[:, i * tok:(i + 1) * tok] = src * mult[:, i:i + 1] + shift[:, i:i + 1]

    for i in range(NP - NX):
        spread(i, out_ref[:, i * tok:(i + 1) * tok])

    @pl.when(outer)
    def _():
        for i in range(NP - NX, NP):
            spread(i, out_ref[:, i * tok:(i + 1) * tok])
        for k in range(NX):
            x_copy(k).wait_send()

    @pl.when(inner)
    def _():
        for k in range(NX):
            x_copy(k).wait_recv()
            spread(NP - NX + k, x_in[k])
        for dz, dv in peers:
            st_copy(2 * v + z - 1, dz, dv).wait_send()


def solution(mesh):
    assert mesh.shape["hid"] == 4 and mesh.shape["vocab"] == 4

    def local_step(h_blk, w_blk, temp_blk, tgt_blk):
        rows, depth = h_blk.shape
        cols = w_blk.shape[1] // 4
        tok = cols // NP
        assert rows == 32 and tok % 128 == 0
        block = (rows, tok)
        vmem, dma = pltpu.VMEM, pltpu.SemaphoreType.DMA
        any_space = pl.BlockSpec(memory_space=pltpu.MemorySpace.HBM)
        in_vmem = pl.BlockSpec(memory_space=pltpu.VMEM)
        table, at_tgt = pl.pallas_call(
            functools.partial(kernel, tok),
            out_shape=(jax.ShapeDtypeStruct((rows, cols), F32), jax.ShapeDtypeStruct((1, rows), F32)),
            in_specs=[any_space, any_space, in_vmem, in_vmem],
            out_specs=(in_vmem, in_vmem),
            scratch_shapes=[
                vmem((rows, depth), BF16),
                vmem((4, depth, tok), BF16),
                vmem((4 * NP, *block), F32),
                vmem((3 * NP, *block), F32),
                vmem((2 * NP, *block), F32),
                vmem((NP, *block), F32),
                vmem((NX, *block), F32),
                vmem((NX, *block), F32),
                vmem((NX, *block), F32),
                vmem((32, 128), F32),
                vmem((32, 128), F32),
                vmem((32, 128), F32),
                vmem((8, 128), F32),
                vmem((8, 128), F32),
                vmem((8, 8, 128), F32),
                dma, dma((4,)),
                dma((RING,)), dma((3 * NP,)), dma((2 * NP,)),
                dma((RING,)), dma((NP,)),
                dma((NX,)), dma((NX,)), dma((NX,)), dma((NX,)),
                dma, dma, dma((16,)), dma((8,)),
            ],
            compiler_params=pltpu.CompilerParams(collective_id=0, has_side_effects=True,
                                                 vmem_limit_bytes=48 * 2 ** 20),
            name="head_cdf",
        )(h_blk, w_blk, temp_blk.reshape(1, rows), tgt_blk.reshape(1, rows))
        return table, at_tgt.reshape(rows)

    return jax.shard_map(local_step, mesh=mesh,
                         in_specs=(P("data", "hid"), P("hid", "vocab"), P("data"), P("data")),
                         out_specs=(P("data", ("vocab", "hid")), P("data")), check_vma=False)
```

```python
import functools

import jax
import jax.numpy as jnp
from jax import lax
from jax.experimental import pallas as pl
from jax.experimental.pallas import tpu as pltpu
from jax.sharding import PartitionSpec as P

MESH = pl.DeviceIdType.MESH
NP = 16
NX = 4
RING = 3
LAG = 3
XSTEP = 2 * NP + 5
VMEM_LIMIT = 67043328 - 2 ** 21 - 2 ** 13
F32 = jnp.float32
BF16 = jnp.bfloat16


def iota(shape, dim):
    return lax.broadcasted_iota(jnp.int32, shape, dim)


def to_col(row):
    n = row.shape[1]
    return jnp.sum(jnp.where(iota((32, n), 0) == iota((32, n), 1), row, 0.0), axis=1, keepdims=True)


def pack_row(m, s, t):
    sub, lane = iota((32, 128), 0), iota((32, 128), 1)
    picked = jnp.where(lane == sub, m, jnp.where(lane == sub + 32, s, jnp.where(lane == sub + 64, t, 0.0)))
    return jnp.sum(picked, axis=0, keepdims=True)


def kernel(tok, h_hbm, w_hbm, temp_hbm, tgt_hbm, out_ref, tgt_out_ref,
           h_buf, temp_buf, tgt_buf, w_buf, part, far_in, side_in, near_in, x_part, x_src, x_in, piece_m, piece_s, piece_t,
           msg_src, msg_in, stats, res_src, res_in,
           h_sem, temp_sem, tgt_sem, w_sem, far_send, far_recv, side_recv, near_send, near_recv, xp_send, xp_recv, x_send, x_recv,
           msg_send, msg_recv, st_send, st_recv, res_send, res_recv, ready):
    z, v = lax.axis_index("hid"), lax.axis_index("vocab")
    outer = (z == 0) | (z == 3)
    inner = (z == 1) | (z == 2)
    far = jnp.where(z < 2, z + 1, z - 1)
    near = jnp.where(z == 1, 0, 3)
    cols = NP * tok
    last = 3 * NP - NX

    def w_load(rel, i, slot):
        owner = jnp.where(z < 2, rel, 3 - rel)
        start = pl.multiple_of(owner * cols + i * tok, tok)
        return pltpu.make_async_copy(w_hbm.at[:, pl.ds(start, tok)], w_buf.at[slot], w_sem.at[slot])

    h_copy = pltpu.make_async_copy(h_hbm, h_buf, h_sem)
    temp_copy = pltpu.make_async_copy(temp_hbm, temp_buf, temp_sem)
    tgt_copy = pltpu.make_async_copy(tgt_hbm, tgt_buf, tgt_sem)
    barrier = pltpu.get_barrier_semaphore()

    def greet(dev):
        pl.semaphore_signal(barrier, inc=1, device_id=dev, device_id_type=MESH)

    greet({"hid": far})

    @pl.when(inner)
    def _():
        greet({"hid": near})

    h_copy.start()
    w_load(3, 0, 0).start()

    @pl.when(inner)
    def _():
        for dv in range(1, 4):
            greet({"vocab": lax.rem(v + dv, 4)})

    temp_copy.start()
    tgt_copy.start()

    def product(rel, i, slot):
        w_load(rel, i, slot).wait()
        part[rel * NP + i] = jnp.dot(h_buf[...], w_buf[slot], preferred_element_type=F32)

        @pl.when(i + 1 < NP)
        def _():
            w_load(rel, i + 1, slot).start()

    def products(i):
        product(0, i, 1)
        product(2, i, 2)
        product(1, i, 3)

        @pl.when(i + 1 < NP)
        def _():
            product(3, i + 1, 0)

    tri = (iota((128, 128), 0) <= iota((128, 128), 1)).astype(BF16)
    piece_m[...] = jnp.zeros_like(piece_m)
    piece_s[...] = jnp.zeros_like(piece_s)
    piece_t[...] = jnp.zeros_like(piece_t)

    def put(ref, lane, value):
        ref[...] = jnp.where(iota((32, 128), 1) == lane, value, ref[...])

    def finish(total, first, lane, store):
        logits = total * temp
        m = jnp.max(logits, axis=1, keepdims=True)
        e = jnp.exp(logits - m)
        n_blk = tok // 128
        terms = []
        for b in range(n_blk):
            blk = e[:, b * 128:(b + 1) * 128]
            hi = blk.astype(BF16)
            rest = blk - hi.astype(F32)
            mid = rest.astype(BF16)
            low = (rest - mid.astype(F32)).astype(BF16)
            terms += [hi, mid, low]
        sums = jnp.dot(jnp.concatenate(terms, axis=0), tri, preferred_element_type=F32)
        carry = jnp.zeros((32, 1), F32)
        hit = jnp.zeros((32, 128), F32)
        pos = tgt - first
        lanes = iota((32, 128), 1).astype(F32)
        for b in range(n_blk):
            s = sums[96 * b:96 * b + 96]
            c = (s[0:32] + s[32:64] + s[64:96]) + carry
            store(b, c)
            hit = hit + jnp.where(lanes == pos - float(b * 128), c, 0.0)
            carry = c[:, 127:128]
        put(piece_m, lane, m)
        put(piece_s, lane, carry)
        put(piece_t, lane, jnp.sum(hit, axis=1, keepdims=True))

    def first_token(owner, i):
        return (((v * 4 + owner) * NP + i) * tok).astype(F32)

    def scan_lanes(x):
        lane = iota((32, 128), 1)
        for shift in (1, 2, 4, 8):
            x = x + jnp.where(lane >= shift, pltpu.roll(x, shift, 1), 0.0)
        return x

    def combine(owner):
        lane = iota((32, 128), 1)
        live = lane < NP
        m_all, s_all, t_all = piece_m[...], piece_s[...], piece_t[...]
        m = jnp.max(jnp.where(live, m_all, m_all[:, 0:1]), axis=1, keepdims=True)
        scale = jnp.where(live, jnp.exp(jnp.where(live, m_all, m) - m), 0.0)
        tot = s_all * scale
        s = jnp.sum(tot, axis=1, keepdims=True)
        low = lane.astype(F32) * float(tok) + first_token(owner, 0)
        t = jnp.sum(jnp.where(low + float(tok) <= tgt, tot, jnp.where(low <= tgt, t_all * scale, 0.0)),
                    axis=1, keepdims=True)
        return pack_row(m, s, t)

    def far_copy(src, t, dst, sems):
        return pltpu.make_async_remote_copy(src_ref=src, dst_ref=dst.at[t], send_sem=far_send.at[lax.rem(t, RING)],
                                            recv_sem=sems.at[t], device_id={"hid": far}, device_id_type=MESH)

    def outer_copy(t):
        i, ph = lax.rem(t, NP), t // NP
        return far_copy(part.at[(3 - ph) * NP + i], t, far_in, far_recv)

    def inner_copy(t):
        return far_copy(far_in.at[t], t, side_in, side_recv)

    def near_copy(g):
        return pltpu.make_async_remote_copy(src_ref=side_in.at[g], dst_ref=near_in.at[g],
                                            send_sem=near_send.at[lax.rem(g, RING)], recv_sem=near_recv.at[g],
                                            device_id={"hid": near}, device_id_type=MESH)

    def x_part_copy(k):
        return pltpu.make_async_remote_copy(src_ref=side_in.at[2 * NP - NX + k], dst_ref=x_part.at[k],
                                            send_sem=xp_send.at[k], recv_sem=xp_recv.at[k],
                                            device_id={"hid": near}, device_id_type=MESH)

    def x_copy(k):
        return pltpu.make_async_remote_copy(src_ref=x_src.at[k], dst_ref=x_in.at[k], send_sem=x_send.at[k],
                                            recv_sem=x_recv.at[k], device_id={"hid": far}, device_id_type=MESH)

    msg_copy = pltpu.make_async_remote_copy(src_ref=msg_src, dst_ref=msg_in, send_sem=msg_send, recv_sem=msg_recv,
                                            device_id={"hid": far}, device_id_type=MESH)

    h_copy.wait()
    product(3, 0, 0)
    for slot, rel in ((1, 0), (2, 2), (3, 1)):
        w_load(rel, 0, slot).start()
    temp_copy.wait()
    tgt_copy.wait()
    temp = to_col(temp_buf[...])
    tgt = to_col(tgt_buf[...].astype(F32))

    @pl.when(outer)
    def _():
        pl.semaphore_wait(barrier, 1)

    @pl.when(inner)
    def _():
        pl.semaphore_wait(barrier, 5)
        pl.semaphore_signal(ready, inc=1, device_id={"hid": far}, device_id_type=MESH)

    def out_store(i):
        def store(b, c):
            out_ref[:, pl.ds(pl.multiple_of(i * tok + b * 128, 128), 128)] = c
        return store

    @pl.when(outer)
    def _():
        def step(t, _):
            i = lax.rem(t, NP)

            @pl.when(t >= RING)
            def _():
                outer_copy(t - RING).wait_send()

            outer_copy(t).start()

            @pl.when(t < NP)
            def _():
                products(i)

            @pl.when((t >= NP) & (t < 2 * NP))
            def _():
                near_copy(i).wait_recv()
                finish(part[i] + near_in[i], first_token(z, i), i, out_store(i))

            @pl.when(t == XSTEP)
            def _():
                for k in range(NX):
                    def store(b, c, k=k):
                        x_src[k, :, b * 128:(b + 1) * 128] = c
                    x_part_copy(k).wait_recv()
                    finish(part[2 * NP - NX + k] + x_part[k], first_token(far, NP - NX + k), NP + k, store)
                rows = [combine(z)]
                for k in range(NX):
                    lane = NP + k
                    rows.append(pack_row(piece_m[:, lane:lane + 1], piece_s[:, lane:lane + 1],
                                         piece_t[:, lane:lane + 1]))
                sub = iota((8, 128), 0)
                tile = jnp.zeros((8, 128), F32)
                for k, row in enumerate(rows):
                    tile = jnp.where(sub == k, row, tile)
                msg_src[...] = tile

            @pl.when(t == XSTEP + 1)
            def _():
                msg_copy.start()

            return ()

        lax.fori_loop(0, last, step, ())
        for k in range(NX):
            x_copy(k).start()
        for k in range(RING):
            outer_copy(last - RING + k).wait_send()
        msg_copy.wait_send()

    @pl.when(inner)
    def _():
        def step(t, _):
            i, ph = lax.rem(t, NP), t // NP
            g = t - LAG
            far_copy(far_in.at[t], t, far_in, far_recv).wait_recv()

            @pl.when((t >= 1) & (t <= 2 * NP))
            def _():
                @pl.when(t - 1 >= RING)
                def _():
                    inner_copy(t - 1 - RING).wait_send()
                inner_copy(t - 1).start()

            @pl.when((g >= 1) & (g <= NP))
            def _():
                @pl.when(g - 1 >= RING)
                def _():
                    near_copy(g - 1 - RING).wait_send()
                near_copy(g - 1).start()

            for k in range(NX):
                @pl.when(g - 1 == 2 * NP - NX + k)
                def _(k=k):
                    x_part_copy(k).start()

            @pl.when(t < 2 * NP)
            def _():
                far_in[t] = far_in[t] + part[(3 - ph) * NP + i]

            @pl.when((g >= 0) & (g < 2 * NP))
            def _():
                far_copy(far_in.at[g], g, side_in, side_recv).wait_recv()

                @pl.when((g < NP) | (g >= 2 * NP - NX))
                def _():
                    side_in[g] = side_in[g] + part[g]

            @pl.when(t < NP)
            def _():
                products(i)

            @pl.when(t >= 2 * NP)
            def _():
                finish(part[NP + i] + side_in[NP + i] + far_in[t], first_token(z, i), i, out_store(i))

            return ()

        lax.fori_loop(0, last, step, ())
        msg_copy.wait_recv()
        msg = msg_in[...]
        for k in range(NX):
            lane = NP - NX + k
            row = msg[k + 1:k + 2]
            put(piece_m, lane, to_col(row))
            put(piece_s, lane, to_col(pltpu.roll(row, 96, 1)))
            put(piece_t, lane, to_col(pltpu.roll(row, 64, 1)))
        mine = combine(z)
        theirs = msg[0:1]
        sub, lane = iota((8, 128), 0), iota((8, 128), 1)
        tile = jnp.where(sub == 0, jnp.where(z == 1, theirs, mine),
                         jnp.where(sub == 1, jnp.where(z == 1, mine, theirs), jnp.where(lane < 32, mine, 0.0)))
        stats[2 * v + z - 1] = tile

    slot = 2 * v + z - 1

    def st_copy(slot, cross, dv):
        return pltpu.make_async_remote_copy(src_ref=stats.at[slot], dst_ref=stats.at[slot],
                                            send_sem=st_send.at[4 * cross + dv], recv_sem=st_recv.at[slot],
                                            device_id={"hid": far if cross else z, "vocab": lax.rem(v + dv, 4)},
                                            device_id_type=MESH)

    peers = [(cross, dv) for cross in (1, 0) for dv in range(4) if cross or dv]
    res_copy = pltpu.make_async_remote_copy(src_ref=res_src, dst_ref=res_in, send_sem=res_send, recv_sem=res_recv,
                                            device_id={"hid": near}, device_id_type=MESH)

    def settle(m_row, s_row, below_row):
        m_col, s_col, below = to_col(m_row), to_col(s_row), to_col(below_row)
        alive = iota((32, 128), 1) < NP
        mult = jnp.exp(jnp.where(alive, piece_m[...], m_col) - m_col)
        totals = jnp.where(alive, piece_s[...] * mult, 0.0)
        return mult / s_col, (below + (scan_lanes(totals) - totals)) / s_col

    def spread(i, src, mult, shift):
        out_ref[:, i * tok:(i + 1) * tok] = src * mult[:, i:i + 1] + shift[:, i:i + 1]

    @pl.when(inner)
    def _():
        pl.semaphore_wait(ready, 1)
        for cross, dv in peers:
            st_copy(slot, cross, dv).start()
        for k in range(RING):
            inner_copy(2 * NP - RING + k).wait_send()
            near_copy(NP - RING + k).wait_send()
        for k in range(NX):
            x_part_copy(k).wait_send()
        for other in range(8):
            @pl.when(slot != other)
            def _(other=other):
                st_copy(other, 0, 1).wait_recv()

        table = stats[...].reshape(64, 128)
        row_id = iota((64, 128), 0)
        m_row = jnp.max(table, axis=0, keepdims=True)
        scale = jnp.exp(table - m_row)
        live = (row_id & 7) < 2
        tot = jnp.where(live, pltpu.roll(table, 96, 1) * scale, 0.0)
        t_val = jnp.where(live, pltpu.roll(table, 64, 1) * scale, 0.0)
        s_row = jnp.sum(tot, axis=0, keepdims=True)

        def below(zz):
            me = v * 16 + (zz // 2) * 8 + lax.rem(zz, 2)
            return jnp.sum(jnp.where(row_id < me, tot, 0.0), axis=0, keepdims=True)

        low = (((row_id >> 3) * 2 + (row_id & 7)) * cols).astype(F32)
        tgt_lanes = jnp.sum(jnp.where(iota((32, 128), 0) == iota((32, 128), 1), tgt, 0.0), axis=0, keepdims=True)
        at_tgt = jnp.sum(jnp.where(low + float(cols) <= tgt_lanes, tot, jnp.where(low <= tgt_lanes, t_val, 0.0)),
                         axis=0, keepdims=True) / s_row
        sub = iota((8, 128), 0)
        res_src[...] = jnp.where(sub == 0, m_row, jnp.where(sub == 1, s_row, jnp.where(sub == 2, below(near), at_tgt)))
        tgt_out_ref[...] = at_tgt[:, 0:32]
        mult, shift = settle(m_row, s_row, below(z))
        res_copy.start()
        for i in range(NP - NX):
            spread(i, out_ref[:, i * tok:(i + 1) * tok], mult, shift)
        for k in range(NX):
            x_copy(k).wait_recv()
            spread(NP - NX + k, x_in[k], mult, shift)
        for cross, dv in peers:
            st_copy(slot, cross, dv).wait_send()
        res_copy.wait_send()

    @pl.when(outer)
    def _():
        res_copy.wait_recv()
        res = res_in[...]
        tgt_out_ref[...] = res[3:4, 0:32]
        mult, shift = settle(res[0:1], res[1:2], res[2:3])
        for i in range(NP):
            spread(i, out_ref[:, i * tok:(i + 1) * tok], mult, shift)
        for k in range(NX):
            x_copy(k).wait_send()


def write_kernel(table_ref, at_tgt_ref, table_hbm, at_tgt_hbm, sems, at_sem):
    copies = [pltpu.make_async_copy(table_ref.at[pl.ds(8 * k, 8)], table_hbm.at[pl.ds(8 * k, 8)], sems.at[k])
              for k in range(4)]
    copies.append(pltpu.make_async_copy(at_tgt_ref, at_tgt_hbm, at_sem))
    for c in copies:
        c.start()
    for c in copies:
        c.wait()


def solution(mesh):
    assert mesh.shape["hid"] == 4 and mesh.shape["vocab"] == 4

    def local_step(h_blk, w_blk, temp_blk, tgt_blk):
        rows, depth = h_blk.shape
        cols = w_blk.shape[1] // 4
        tok = cols // NP
        assert rows == 32 and tok % 128 == 0
        block = (rows, tok)
        vmem, dma = pltpu.VMEM, pltpu.SemaphoreType.DMA
        hbm = pl.BlockSpec(memory_space=pltpu.MemorySpace.HBM)
        in_vmem = pl.BlockSpec(memory_space=pltpu.VMEM)
        shapes = (jax.ShapeDtypeStruct((rows, cols), F32), jax.ShapeDtypeStruct((1, rows), F32))
        table, at_tgt = pl.pallas_call(
            functools.partial(kernel, tok),
            out_shape=(pltpu.VMEM((rows, cols), F32), pltpu.VMEM((1, rows), F32)),
            in_specs=[hbm] * 4,
            out_specs=(in_vmem, in_vmem),
            scratch_shapes=[
                vmem((rows, depth), BF16), vmem((1, rows), F32), vmem((1, rows), jnp.int32),
                vmem((4, depth, tok), BF16),
                vmem((4 * NP, *block), F32),
                vmem((3 * NP, *block), F32),
                vmem((2 * NP, *block), F32),
                vmem((NP, *block), F32),
                vmem((NX, *block), F32),
                vmem((NX, *block), F32),
                vmem((NX, *block), F32),
                vmem((32, 128), F32),
                vmem((32, 128), F32),
                vmem((32, 128), F32),
                vmem((8, 128), F32), vmem((8, 128), F32), vmem((8, 8, 128), F32),
                vmem((8, 128), F32), vmem((8, 128), F32),
                dma, dma, dma, dma((4,)),
                dma((RING,)), dma((3 * NP,)), dma((2 * NP,)),
                dma((RING,)), dma((NP,)),
                dma((NX,)), dma((NX,)), dma((NX,)), dma((NX,)),
                dma, dma, dma((8,)), dma((8,)), dma, dma, pltpu.SemaphoreType.REGULAR,
            ],
            compiler_params=pltpu.CompilerParams(collective_id=0, has_side_effects=True, vmem_limit_bytes=VMEM_LIMIT),
            name="head_cdf",
        )(h_blk, w_blk, temp_blk.reshape(1, rows), tgt_blk.reshape(1, rows))
        table, at_tgt = pl.pallas_call(
            write_kernel,
            out_shape=shapes,
            in_specs=[in_vmem, in_vmem],
            out_specs=(hbm, hbm),
            scratch_shapes=[dma((4,)), dma],
            compiler_params=pltpu.CompilerParams(vmem_limit_bytes=2 ** 20),
            name="write",
        )(table, at_tgt)
        return table, at_tgt.reshape(rows)

    return jax.shard_map(local_step, mesh=mesh,
                         in_specs=(P("data", "hid"), P("hid", "vocab"), P("data"), P("data")),
                         out_specs=(P("data", ("vocab", "hid")), P("data")), check_vma=False)
```

```python
import functools

import jax
import jax.numpy as jnp
from jax import lax
from jax.experimental import pallas as pl
from jax.experimental.pallas import tpu as pltpu
from jax.sharding import PartitionSpec as P

MESH = pl.DeviceIdType.MESH
NP = 16
NX = 6
RING = 4
LAG = 4
XSTEP = 2 * NP - 3
SUB = 2
VMEM_LIMIT = 67043328 - 2 ** 21 - 2 ** 13
F32 = jnp.float32
BF16 = jnp.bfloat16


def iota(shape, dim):
    return lax.broadcasted_iota(jnp.int32, shape, dim)


def to_col(row):
    n = row.shape[1]
    return jnp.sum(jnp.where(iota((32, n), 0) == iota((32, n), 1), row, 0.0), axis=1, keepdims=True)


def pack_row(m, s, t):
    sub, lane = iota((32, 128), 0), iota((32, 128), 1)
    picked = jnp.where(lane == sub, m, jnp.where(lane == sub + 32, s, jnp.where(lane == sub + 64, t, 0.0)))
    return jnp.sum(picked, axis=0, keepdims=True)


def kernel(tok, h_hbm, w_hbm, temp_hbm, tgt_hbm, out_ref, tgt_out_ref,
           h_buf, temp_buf, tgt_buf, w_buf, part, far_in, side_in, near_in, x_part, x_src, x_in, piece_m, piece_s, piece_t,
           msg_src, msg_in, stats, res_src, res_in,
           h_sem, temp_sem, tgt_sem, w_sem, sub_w, sub_send, sub_recv, far_send, far_recv, side_recv, near_send, near_recv, xp_send, xp_recv, x_send, x_recv,
           msg_send, msg_recv, st_send, st_recv, res_send, res_recv, ready):
    z, v = lax.axis_index("hid"), lax.axis_index("vocab")
    outer = (z == 0) | (z == 3)
    inner = (z == 1) | (z == 2)
    far = jnp.where(z < 2, z + 1, z - 1)
    near = jnp.where(z == 1, 0, 3)
    cols = NP * tok
    part_tok = tok // SUB
    last = 3 * NP - NX

    def w_load(rel, i, slot):
        owner = jnp.where(z < 2, rel, 3 - rel)
        start = pl.multiple_of(owner * cols + i * tok, tok)
        return pltpu.make_async_copy(w_hbm.at[:, pl.ds(start, tok)], w_buf.at[slot], w_sem.at[slot])

    h_copy = pltpu.make_async_copy(h_hbm, h_buf, h_sem)
    temp_copy = pltpu.make_async_copy(temp_hbm, temp_buf, temp_sem)
    tgt_copy = pltpu.make_async_copy(tgt_hbm, tgt_buf, tgt_sem)
    barrier = pltpu.get_barrier_semaphore()

    def greet(dev):
        pl.semaphore_signal(barrier, inc=1, device_id=dev, device_id_type=MESH)

    def part_of(k):
        return pl.ds(k * part_tok, part_tok)

    def sub_load(k):
        owner = jnp.where(z < 2, 3, 0)
        start = pl.multiple_of(owner * cols + k * part_tok, part_tok)
        return pltpu.make_async_copy(w_hbm.at[:, pl.ds(start, part_tok)], w_buf.at[0, :, part_of(k)], sub_w.at[k])

    @pl.when(inner)
    def _():
        greet({"hid": near})

    h_copy.start()
    for k in range(SUB):
        sub_load(k).start()
    greet({"hid": far})

    @pl.when(inner)
    def _():
        for dv in range(1, 4):
            greet({"vocab": lax.rem(v + dv, 4)})

    temp_copy.start()
    tgt_copy.start()

    def product(rel, i, slot):
        w_load(rel, i, slot).wait()
        part[rel * NP + i] = jnp.dot(h_buf[...], w_buf[slot], preferred_element_type=F32)

        @pl.when(i + 1 < NP)
        def _():
            w_load(rel, i + 1, slot).start()

    def products(i):
        product(0, i, 1)
        product(2, i, 2)
        product(1, i, 3)

        @pl.when(i + 1 < NP)
        def _():
            product(3, i + 1, 0)

    def sub_product(k):
        sub_load(k).wait()
        part[3 * NP, :, part_of(k)] = jnp.dot(h_buf[...], w_buf[0, :, part_of(k)], preferred_element_type=F32)

    def sub_copy(k):
        return pltpu.make_async_remote_copy(src_ref=part.at[3 * NP, :, part_of(k)], dst_ref=far_in.at[0, :, part_of(k)],
                                            send_sem=sub_send.at[k], recv_sem=sub_recv.at[k],
                                            device_id={"hid": far}, device_id_type=MESH)

    tri = (iota((128, 128), 0) <= iota((128, 128), 1)).astype(BF16)
    piece_m[...] = jnp.zeros_like(piece_m)
    piece_s[...] = jnp.zeros_like(piece_s)
    piece_t[...] = jnp.zeros_like(piece_t)

    def put(ref, lane, value):
        ref[...] = jnp.where(iota((32, 128), 1) == lane, value, ref[...])

    def finish(total, first, lane, store):
        logits = total * temp
        m = jnp.max(logits, axis=1, keepdims=True)
        e = jnp.exp(logits - m)
        n_blk = tok // 128
        terms = []
        for b in range(n_blk):
            blk = e[:, b * 128:(b + 1) * 128]
            hi = blk.astype(BF16)
            rest = blk - hi.astype(F32)
            mid = rest.astype(BF16)
            low = (rest - mid.astype(F32)).astype(BF16)
            terms += [hi, mid, low]
        sums = jnp.dot(jnp.concatenate(terms, axis=0), tri, preferred_element_type=F32)
        carry = jnp.zeros((32, 1), F32)
        hit = jnp.zeros((32, 128), F32)
        pos = tgt - first
        lanes = iota((32, 128), 1).astype(F32)
        for b in range(n_blk):
            s = sums[96 * b:96 * b + 96]
            c = (s[0:32] + s[32:64] + s[64:96]) + carry
            store(b, c)
            hit = hit + jnp.where(lanes == pos - float(b * 128), c, 0.0)
            carry = c[:, 127:128]
        put(piece_m, lane, m)
        put(piece_s, lane, carry)
        put(piece_t, lane, jnp.sum(hit, axis=1, keepdims=True))

    def first_token(owner, i):
        return (((v * 4 + owner) * NP + i) * tok).astype(F32)

    def scan_lanes(x):
        lane = iota((32, 128), 1)
        for shift in (1, 2, 4, 8):
            x = x + jnp.where(lane >= shift, pltpu.roll(x, shift, 1), 0.0)
        return x

    def combine(owner):
        lane = iota((32, 128), 1)
        live = lane < NP
        m_all, s_all, t_all = piece_m[...], piece_s[...], piece_t[...]
        m = jnp.max(jnp.where(live, m_all, m_all[:, 0:1]), axis=1, keepdims=True)
        scale = jnp.where(live, jnp.exp(jnp.where(live, m_all, m) - m), 0.0)
        tot = s_all * scale
        s = jnp.sum(tot, axis=1, keepdims=True)
        low = lane.astype(F32) * float(tok) + first_token(owner, 0)
        t = jnp.sum(jnp.where(low + float(tok) <= tgt, tot, jnp.where(low <= tgt, t_all * scale, 0.0)),
                    axis=1, keepdims=True)
        return pack_row(m, s, t)

    def far_copy(src, t, dst, sems):
        return pltpu.make_async_remote_copy(src_ref=src, dst_ref=dst.at[t], send_sem=far_send.at[lax.rem(t, RING)],
                                            recv_sem=sems.at[t], device_id={"hid": far}, device_id_type=MESH)

    def part_index(t):
        i, ph = lax.rem(t, NP), t // NP
        return (3 - ph) * NP + jnp.where(ph == 1, lax.rem(i + NP - NX, NP), i)

    def outer_copy(t):
        return far_copy(part.at[part_index(t)], t, far_in, far_recv)

    def inner_copy(t):
        return far_copy(far_in.at[t], t, side_in, side_recv)

    def near_copy(g):
        return pltpu.make_async_remote_copy(src_ref=side_in.at[g], dst_ref=near_in.at[g],
                                            send_sem=near_send.at[lax.rem(g, RING)], recv_sem=near_recv.at[g],
                                            device_id={"hid": near}, device_id_type=MESH)

    def x_part_copy(k):
        return pltpu.make_async_remote_copy(src_ref=side_in.at[NP + k], dst_ref=x_part.at[k],
                                            send_sem=xp_send.at[k], recv_sem=xp_recv.at[k],
                                            device_id={"hid": near}, device_id_type=MESH)

    def x_copy(k):
        return pltpu.make_async_remote_copy(src_ref=x_src.at[k], dst_ref=x_in.at[k], send_sem=x_send.at[k],
                                            recv_sem=x_recv.at[k], device_id={"hid": far}, device_id_type=MESH)

    msg_copy = pltpu.make_async_remote_copy(src_ref=msg_src, dst_ref=msg_in, send_sem=msg_send, recv_sem=msg_recv,
                                            device_id={"hid": far}, device_id_type=MESH)

    h_copy.wait()
    for k in range(SUB):
        sub_product(k)
        if k == 0:
            for slot, rel in ((1, 0), (2, 2), (3, 1)):
                w_load(rel, 0, slot).start()

            @pl.when(outer)
            def _():
                pl.semaphore_wait(barrier, 1)

        @pl.when(outer)
        def _(k=k):
            sub_copy(k).start()

    w_load(3, 1, 0).start()
    temp_copy.wait()
    tgt_copy.wait()
    temp = to_col(temp_buf[...])
    tgt = to_col(tgt_buf[...].astype(F32))

    @pl.when(inner)
    def _():
        pl.semaphore_wait(barrier, 5)
        pl.semaphore_signal(ready, inc=1, device_id={"hid": far}, device_id_type=MESH)

    def out_store(i):
        def store(b, c):
            out_ref[:, pl.ds(pl.multiple_of(i * tok + b * 128, 128), 128)] = c
        return store

    @pl.when(outer)
    def _():
        def step(t, _):
            i = lax.rem(t, NP)

            @pl.when(t > RING)
            def _():
                outer_copy(t - RING).wait_send()

            @pl.when(t > 0)
            def _():
                outer_copy(t).start()

            @pl.when(t < NP)
            def _():
                products(i)

            @pl.when((t >= NP) & (t < 2 * NP))
            def _():
                near_copy(i).wait_recv()
                finish(part[i] + near_in[i], first_token(z, i), i, out_store(i))

            @pl.when((t >= XSTEP) & (t < XSTEP + NX))
            def _():
                k = t - XSTEP

                def store(b, c):
                    x_src[k, :, b * 128:(b + 1) * 128] = c
                x_part_copy(k).wait_recv()
                finish(part[2 * NP - NX + k] + x_part[k], first_token(far, NP - NX + k), NP + k, store)

            @pl.when(t == XSTEP + NX)
            def _():
                sub = iota((8, 128), 0)
                tile = jnp.where(sub == 0, combine(z), 0.0)
                for k in range(NX):
                    lane = NP + k
                    row = pack_row(piece_m[:, lane:lane + 1], piece_s[:, lane:lane + 1], piece_t[:, lane:lane + 1])
                    tile = jnp.where(sub == k + 1, row, tile)
                msg_src[...] = tile

            @pl.when(t == XSTEP + NX + 1)
            def _():
                msg_copy.start()

            return ()

        lax.fori_loop(0, last, step, ())
        for k in range(NX):
            x_copy(k).start()
        for k in range(SUB):
            sub_copy(k).wait_send()
        for k in range(RING):
            outer_copy(last - RING + k).wait_send()
        msg_copy.wait_send()

    @pl.when(inner)
    def _():
        def step(t, _):
            i = lax.rem(t, NP)
            g = t - LAG

            @pl.when(t == 0)
            def _():
                for k in range(SUB):
                    sub_copy(k).wait_recv()

            @pl.when(t > 0)
            def _():
                far_copy(far_in.at[t], t, far_in, far_recv).wait_recv()

            @pl.when((t >= 1) & (t <= 2 * NP))
            def _():
                @pl.when(t - 1 >= RING)
                def _():
                    inner_copy(t - 1 - RING).wait_send()
                inner_copy(t - 1).start()

            @pl.when((g >= 1) & (g <= NP))
            def _():
                @pl.when(g - 1 >= RING)
                def _():
                    near_copy(g - 1 - RING).wait_send()
                near_copy(g - 1).start()

            for k in range(NX):
                @pl.when(g - 1 == NP + k)
                def _(k=k):
                    x_part_copy(k).start()

            @pl.when(t < 2 * NP)
            def _():
                far_in[t] = far_in[t] + part[part_index(t)]

            @pl.when((g >= 0) & (g < 2 * NP))
            def _():
                far_copy(far_in.at[g], g, side_in, side_recv).wait_recv()

                @pl.when(g < NP + NX)
                def _():
                    side_in[g] = side_in[g] + part[jnp.where(g < NP, g, g + NP - NX)]

            @pl.when(t < NP)
            def _():
                products(i)

            @pl.when(t >= 2 * NP)
            def _():
                finish(part[NP + i] + side_in[NP + NX + i] + far_in[t], first_token(z, i), i, out_store(i))

            return ()

        lax.fori_loop(0, last, step, ())
        msg_copy.wait_recv()
        msg = msg_in[...]
        for k in range(NX):
            lane = NP - NX + k
            row = msg[k + 1:k + 2]
            put(piece_m, lane, to_col(row))
            put(piece_s, lane, to_col(pltpu.roll(row, 96, 1)))
            put(piece_t, lane, to_col(pltpu.roll(row, 64, 1)))
        mine = combine(z)
        theirs = msg[0:1]
        sub, lane = iota((8, 128), 0), iota((8, 128), 1)
        tile = jnp.where(sub == 0, jnp.where(z == 1, theirs, mine),
                         jnp.where(sub == 1, jnp.where(z == 1, mine, theirs), jnp.where(lane < 32, mine, 0.0)))
        stats[2 * v + z - 1] = tile

    slot = 2 * v + z - 1

    def st_copy(slot, cross, dv):
        return pltpu.make_async_remote_copy(src_ref=stats.at[slot], dst_ref=stats.at[slot],
                                            send_sem=st_send.at[4 * cross + dv], recv_sem=st_recv.at[slot],
                                            device_id={"hid": far if cross else z, "vocab": lax.rem(v + dv, 4)},
                                            device_id_type=MESH)

    peers = [(cross, dv) for cross in (1, 0) for dv in range(4) if cross or dv]
    res_copy = pltpu.make_async_remote_copy(src_ref=res_src, dst_ref=res_in, send_sem=res_send, recv_sem=res_recv,
                                            device_id={"hid": near}, device_id_type=MESH)

    def settle(m_row, s_row, below_row):
        m_col, s_col, below = to_col(m_row), to_col(s_row), to_col(below_row)
        alive = iota((32, 128), 1) < NP
        mult = jnp.exp(jnp.where(alive, piece_m[...], m_col) - m_col)
        totals = jnp.where(alive, piece_s[...] * mult, 0.0)
        return mult / s_col, (below + (scan_lanes(totals) - totals)) / s_col

    def spread(i, src, mult, shift):
        out_ref[:, i * tok:(i + 1) * tok] = src * mult[:, i:i + 1] + shift[:, i:i + 1]

    @pl.when(inner)
    def _():
        pl.semaphore_wait(ready, 1)
        for cross, dv in peers:
            st_copy(slot, cross, dv).start()
        for k in range(RING):
            inner_copy(2 * NP - RING + k).wait_send()
            near_copy(NP - RING + k).wait_send()
        for k in range(NX):
            x_part_copy(k).wait_send()
        for other in range(8):
            @pl.when(slot != other)
            def _(other=other):
                st_copy(other, 0, 1).wait_recv()

        table = stats[...].reshape(64, 128)
        row_id = iota((64, 128), 0)
        m_row = jnp.max(table, axis=0, keepdims=True)
        scale = jnp.exp(table - m_row)
        live = (row_id & 7) < 2
        tot = jnp.where(live, pltpu.roll(table, 96, 1) * scale, 0.0)
        t_val = jnp.where(live, pltpu.roll(table, 64, 1) * scale, 0.0)
        s_row = jnp.sum(tot, axis=0, keepdims=True)

        def below(zz):
            me = v * 16 + (zz // 2) * 8 + lax.rem(zz, 2)
            return jnp.sum(jnp.where(row_id < me, tot, 0.0), axis=0, keepdims=True)

        low = (((row_id >> 3) * 2 + (row_id & 7)) * cols).astype(F32)
        tgt_lanes = jnp.sum(jnp.where(iota((32, 128), 0) == iota((32, 128), 1), tgt, 0.0), axis=0, keepdims=True)
        at_tgt = jnp.sum(jnp.where(low + float(cols) <= tgt_lanes, tot, jnp.where(low <= tgt_lanes, t_val, 0.0)),
                         axis=0, keepdims=True) / s_row
        sub = iota((8, 128), 0)
        res_src[...] = jnp.where(sub == 0, m_row, jnp.where(sub == 1, s_row, jnp.where(sub == 2, below(near), at_tgt)))
        tgt_out_ref[...] = at_tgt[:, 0:32]
        mult, shift = settle(m_row, s_row, below(z))
        res_copy.start()
        for i in range(NP - NX):
            spread(i, out_ref[:, i * tok:(i + 1) * tok], mult, shift)
        for k in range(NX):
            x_copy(k).wait_recv()
            spread(NP - NX + k, x_in[k], mult, shift)
        for cross, dv in peers:
            st_copy(slot, cross, dv).wait_send()
        res_copy.wait_send()

    @pl.when(outer)
    def _():
        res_copy.wait_recv()
        res = res_in[...]
        tgt_out_ref[...] = res[3:4, 0:32]
        mult, shift = settle(res[0:1], res[1:2], res[2:3])
        for i in range(NP):
            spread(i, out_ref[:, i * tok:(i + 1) * tok], mult, shift)
        for k in range(NX):
            x_copy(k).wait_send()


def write_kernel(table_ref, at_tgt_ref, table_hbm, at_tgt_hbm, sems, at_sem):
    copies = [pltpu.make_async_copy(table_ref.at[pl.ds(8 * k, 8)], table_hbm.at[pl.ds(8 * k, 8)], sems.at[k])
              for k in range(4)]
    copies.append(pltpu.make_async_copy(at_tgt_ref, at_tgt_hbm, at_sem))
    for c in copies:
        c.start()
    for c in copies:
        c.wait()


def solution(mesh):
    assert mesh.shape["hid"] == 4 and mesh.shape["vocab"] == 4

    def local_step(h_blk, w_blk, temp_blk, tgt_blk):
        rows, depth = h_blk.shape
        cols = w_blk.shape[1] // 4
        tok = cols // NP
        assert rows == 32 and tok % 128 == 0
        block = (rows, tok)
        vmem, dma = pltpu.VMEM, pltpu.SemaphoreType.DMA
        hbm = pl.BlockSpec(memory_space=pltpu.MemorySpace.HBM)
        in_vmem = pl.BlockSpec(memory_space=pltpu.VMEM)
        shapes = (jax.ShapeDtypeStruct((rows, cols), F32), jax.ShapeDtypeStruct((1, rows), F32))
        table, at_tgt = pl.pallas_call(
            functools.partial(kernel, tok),
            out_shape=(pltpu.VMEM((rows, cols), F32), pltpu.VMEM((1, rows), F32)),
            in_specs=[hbm] * 4,
            out_specs=(in_vmem, in_vmem),
            scratch_shapes=[
                vmem((rows, depth), BF16), vmem((1, rows), F32), vmem((1, rows), jnp.int32),
                vmem((4, depth, tok), BF16),
                vmem((4 * NP, *block), F32),
                vmem((3 * NP, *block), F32),
                vmem((2 * NP, *block), F32),
                vmem((NP, *block), F32),
                vmem((NX, *block), F32),
                vmem((NX, *block), F32),
                vmem((NX, *block), F32),
                vmem((32, 128), F32),
                vmem((32, 128), F32),
                vmem((32, 128), F32),
                vmem((8, 128), F32), vmem((8, 128), F32), vmem((8, 8, 128), F32),
                vmem((8, 128), F32), vmem((8, 128), F32),
                dma, dma, dma, dma((4,)), dma((SUB,)), dma((SUB,)), dma((SUB,)),
                dma((RING,)), dma((3 * NP,)), dma((2 * NP,)),
                dma((RING,)), dma((NP,)),
                dma((NX,)), dma((NX,)), dma((NX,)), dma((NX,)),
                dma, dma, dma((8,)), dma((8,)), dma, dma, pltpu.SemaphoreType.REGULAR,
            ],
            compiler_params=pltpu.CompilerParams(collective_id=0, has_side_effects=True, vmem_limit_bytes=VMEM_LIMIT),
            name="head_cdf",
        )(h_blk, w_blk, temp_blk.reshape(1, rows), tgt_blk.reshape(1, rows))
        table, at_tgt = pl.pallas_call(
            write_kernel,
            out_shape=shapes,
            in_specs=[in_vmem, in_vmem],
            out_specs=(hbm, hbm),
            scratch_shapes=[dma((4,)), dma],
            compiler_params=pltpu.CompilerParams(vmem_limit_bytes=2 ** 20),
            name="write",
        )(table, at_tgt)
        return table, at_tgt.reshape(rows)

    return jax.shard_map(local_step, mesh=mesh,
                         in_specs=(P("data", "hid"), P("hid", "vocab"), P("data"), P("data")),
                         out_specs=(P("data", ("vocab", "hid")), P("data")), check_vma=False)
```

```python
import functools

import jax
import jax.numpy as jnp
from jax import lax
from jax.experimental import pallas as pl
from jax.experimental.pallas import tpu as pltpu
from jax.sharding import PartitionSpec as P

MESH = pl.DeviceIdType.MESH
NP = 16
NX = 6
RING = 2
LAG = 4
XSTEP = 2 * NP - 3
SUB = 2
AHEAD = 2
VMEM_LIMIT = 67043328 - 2 ** 21 - 2 ** 13
F32 = jnp.float32
BF16 = jnp.bfloat16


def iota(shape, dim):
    return lax.broadcasted_iota(jnp.int32, shape, dim)


def to_col(row):
    n = row.shape[1]
    return jnp.sum(jnp.where(iota((32, n), 0) == iota((32, n), 1), row, 0.0), axis=1, keepdims=True)


def pack_row(m, s, t):
    sub, lane = iota((32, 128), 0), iota((32, 128), 1)
    picked = jnp.where(lane == sub, m, jnp.where(lane == sub + 32, s, jnp.where(lane == sub + 64, t, 0.0)))
    return jnp.sum(picked, axis=0, keepdims=True)


def kernel(tok, h_hbm, w_hbm, temp_hbm, tgt_hbm, out_ref, tgt_out_ref,
           h_buf, temp_buf, tgt_buf, w_buf, part, far_in, side_in, near_in, x_part, x_src, x_in, piece_m, piece_s, piece_t,
           msg_src, msg_in, stats, res_src, res_in,
           h_sem, temp_sem, tgt_sem, w_sem, sub_w, sub_send, sub_recv, far_send, far_recv, side_recv, near_send, near_recv, xp_send, xp_recv, x_send, x_recv,
           msg_send, msg_recv, st_send, st_recv, res_send, res_recv, ready):
    z, v = lax.axis_index("hid"), lax.axis_index("vocab")
    outer = (z == 0) | (z == 3)
    inner = (z == 1) | (z == 2)
    far = jnp.where(z < 2, z + 1, z - 1)
    near = jnp.where(z == 1, 0, 3)
    cols = NP * tok
    last = 3 * NP - NX

    def w_load(rel, i, lane):
        slot = lax.rem(i, AHEAD) * 4 + lane
        owner = jnp.where(z < 2, rel, 3 - rel)
        start = pl.multiple_of(owner * cols + i * tok, tok)
        return pltpu.make_async_copy(w_hbm.at[:, pl.ds(start, tok)], w_buf.at[slot], w_sem.at[slot])

    h_copy = pltpu.make_async_copy(h_hbm, h_buf, h_sem)
    temp_copy = pltpu.make_async_copy(temp_hbm, temp_buf, temp_sem)
    tgt_copy = pltpu.make_async_copy(tgt_hbm, tgt_buf, tgt_sem)
    barrier = pltpu.get_barrier_semaphore()

    def greet(dev):
        pl.semaphore_signal(barrier, inc=1, device_id=dev, device_id_type=MESH)

    def part_of(k):
        return pl.ds(0, tok // 4) if k == 0 else pl.ds(tok // 4, tok - tok // 4)

    def sub_load(k):
        owner = jnp.where(z < 2, 3, 0)
        at = part_of(k)
        start = pl.multiple_of(owner * cols + at.start, tok // 4)
        return pltpu.make_async_copy(w_hbm.at[:, pl.ds(start, at.size)], w_buf.at[0, :, at], sub_w.at[k])

    @pl.when(inner)
    def _():
        greet({"hid": near})

    h_copy.start()
    for k in range(SUB):
        sub_load(k).start()
    greet({"hid": far})

    @pl.when(inner)
    def _():
        for dv in range(1, 4):
            greet({"vocab": lax.rem(v + dv, 4)})

    temp_copy.start()
    tgt_copy.start()

    def product(rel, i, lane):
        w_load(rel, i, lane).wait()
        part[rel * NP + i] = jnp.dot(h_buf[...], w_buf[lax.rem(i, AHEAD) * 4 + lane], preferred_element_type=F32)

        @pl.when(i + AHEAD < NP)
        def _():
            w_load(rel, i + AHEAD, lane).start()

    def products(i):
        product(0, i, 1)
        product(2, i, 2)
        product(1, i, 3)

        @pl.when(i + 1 < NP)
        def _():
            product(3, i + 1, 0)

    def sub_product(k):
        sub_load(k).wait()
        part[3 * NP, :, part_of(k)] = jnp.dot(h_buf[...], w_buf[0, :, part_of(k)], preferred_element_type=F32)

    def sub_copy(k):
        return pltpu.make_async_remote_copy(src_ref=part.at[3 * NP, :, part_of(k)], dst_ref=far_in.at[0, :, part_of(k)],
                                            send_sem=sub_send.at[k], recv_sem=sub_recv.at[k],
                                            device_id={"hid": far}, device_id_type=MESH)

    tri = (iota((128, 128), 0) <= iota((128, 128), 1)).astype(BF16)
    piece_m[...] = jnp.zeros_like(piece_m)
    piece_s[...] = jnp.zeros_like(piece_s)
    piece_t[...] = jnp.zeros_like(piece_t)

    def put(ref, lane, value):
        ref[...] = jnp.where(iota((32, 128), 1) == lane, value, ref[...])

    def finish(total, first, lane, store):
        logits = total * temp
        m = jnp.max(logits, axis=1, keepdims=True)
        e = jnp.exp(logits - m)
        n_blk = tok // 128
        terms = []
        for b in range(n_blk):
            blk = e[:, b * 128:(b + 1) * 128]
            hi = blk.astype(BF16)
            rest = blk - hi.astype(F32)
            mid = rest.astype(BF16)
            low = (rest - mid.astype(F32)).astype(BF16)
            terms += [hi, mid, low]
        sums = jnp.dot(jnp.concatenate(terms, axis=0), tri, preferred_element_type=F32)
        carry = jnp.zeros((32, 1), F32)
        hit = jnp.zeros((32, 128), F32)
        pos = tgt - first
        lanes = iota((32, 128), 1).astype(F32)
        for b in range(n_blk):
            s = sums[96 * b:96 * b + 96]
            c = (s[0:32] + s[32:64] + s[64:96]) + carry
            store(b, c)
            hit = hit + jnp.where(lanes == pos - float(b * 128), c, 0.0)
            carry = c[:, 127:128]
        put(piece_m, lane, m)
        put(piece_s, lane, carry)
        put(piece_t, lane, jnp.sum(hit, axis=1, keepdims=True))

    def first_token(owner, i):
        return (((v * 4 + owner) * NP + i) * tok).astype(F32)

    def scan_lanes(x):
        lane = iota((32, 128), 1)
        for shift in (1, 2, 4, 8):
            x = x + jnp.where(lane >= shift, pltpu.roll(x, shift, 1), 0.0)
        return x

    def combine(owner):
        lane = iota((32, 128), 1)
        live = lane < NP
        m_all, s_all, t_all = piece_m[...], piece_s[...], piece_t[...]
        m = jnp.max(jnp.where(live, m_all, m_all[:, 0:1]), axis=1, keepdims=True)
        scale = jnp.where(live, jnp.exp(jnp.where(live, m_all, m) - m), 0.0)
        tot = s_all * scale
        s = jnp.sum(tot, axis=1, keepdims=True)
        low = lane.astype(F32) * float(tok) + first_token(owner, 0)
        t = jnp.sum(jnp.where(low + float(tok) <= tgt, tot, jnp.where(low <= tgt, t_all * scale, 0.0)),
                    axis=1, keepdims=True)
        return pack_row(m, s, t)

    def far_copy(src, t, dst, sems):
        return pltpu.make_async_remote_copy(src_ref=src, dst_ref=dst.at[t], send_sem=far_send.at[lax.rem(t, RING)],
                                            recv_sem=sems.at[t], device_id={"hid": far}, device_id_type=MESH)

    def part_index(t):
        i, ph = lax.rem(t, NP), t // NP
        return (3 - ph) * NP + jnp.where(ph == 1, lax.rem(i + NP - NX, NP), i)

    def outer_copy(t):
        return far_copy(part.at[part_index(t)], t, far_in, far_recv)

    def inner_copy(t):
        return far_copy(far_in.at[t], t, side_in, side_recv)

    def near_copy(g):
        return pltpu.make_async_remote_copy(src_ref=side_in.at[g], dst_ref=near_in.at[g],
                                            send_sem=near_send.at[lax.rem(g, RING)], recv_sem=near_recv.at[g],
                                            device_id={"hid": near}, device_id_type=MESH)

    def x_part_copy(k):
        return pltpu.make_async_remote_copy(src_ref=side_in.at[NP + k], dst_ref=x_part.at[k],
                                            send_sem=xp_send.at[k], recv_sem=xp_recv.at[k],
                                            device_id={"hid": near}, device_id_type=MESH)

    def x_copy(k):
        return pltpu.make_async_remote_copy(src_ref=x_src.at[k], dst_ref=x_in.at[k], send_sem=x_send.at[k],
                                            recv_sem=x_recv.at[k], device_id={"hid": far}, device_id_type=MESH)

    msg_copy = pltpu.make_async_remote_copy(src_ref=msg_src, dst_ref=msg_in, send_sem=msg_send, recv_sem=msg_recv,
                                            device_id={"hid": far}, device_id_type=MESH)

    h_copy.wait()
    for k in range(SUB):
        sub_product(k)
        if k == 0:
            for i in range(AHEAD):
                for lane, rel in ((0, 3), (1, 0), (2, 2), (3, 1)):
                    if i or lane:
                        w_load(rel, i, lane).start()

            @pl.when(outer)
            def _():
                pl.semaphore_wait(barrier, 1)

        @pl.when(outer)
        def _(k=k):
            sub_copy(k).start()

    w_load(3, AHEAD, 0).start()
    temp_copy.wait()
    tgt_copy.wait()
    temp = to_col(temp_buf[...])
    tgt = to_col(tgt_buf[...].astype(F32))

    @pl.when(inner)
    def _():
        pl.semaphore_wait(barrier, 5)
        pl.semaphore_signal(ready, inc=1, device_id={"hid": far}, device_id_type=MESH)

    def out_store(i):
        def store(b, c):
            out_ref[:, pl.ds(pl.multiple_of(i * tok + b * 128, 128), 128)] = c
        return store

    @pl.when(outer)
    def _():
        def step(t, _):
            i = lax.rem(t, NP)

            @pl.when(t > RING)
            def _():
                outer_copy(t - RING).wait_send()

            @pl.when(t > 0)
            def _():
                outer_copy(t).start()

            @pl.when(t < NP)
            def _():
                products(i)

            @pl.when((t >= NP) & (t < 2 * NP))
            def _():
                near_copy(i).wait_recv()
                finish(part[i] + near_in[i], first_token(z, i), i, out_store(i))

            @pl.when((t >= XSTEP) & (t < XSTEP + NX))
            def _():
                k = t - XSTEP

                def store(b, c):
                    x_src[k, :, b * 128:(b + 1) * 128] = c
                x_part_copy(k).wait_recv()
                finish(part[2 * NP - NX + k] + x_part[k], first_token(far, NP - NX + k), NP + k, store)

            @pl.when(t == XSTEP + NX)
            def _():
                sub = iota((8, 128), 0)
                tile = jnp.where(sub == 0, combine(z), 0.0)
                for k in range(NX):
                    lane = NP + k
                    row = pack_row(piece_m[:, lane:lane + 1], piece_s[:, lane:lane + 1], piece_t[:, lane:lane + 1])
                    tile = jnp.where(sub == k + 1, row, tile)
                msg_src[...] = tile

            @pl.when(t == XSTEP + NX + 1)
            def _():
                msg_copy.start()

            return ()

        lax.fori_loop(0, last, step, ())
        for k in range(NX):
            x_copy(k).start()
        for k in range(SUB):
            sub_copy(k).wait_send()
        for k in range(RING):
            outer_copy(last - RING + k).wait_send()
        msg_copy.wait_send()

    @pl.when(inner)
    def _():
        def step(t, _):
            i = lax.rem(t, NP)
            g = t - LAG

            @pl.when(t == 0)
            def _():
                for k in range(SUB):
                    sub_copy(k).wait_recv()

            @pl.when(t > 0)
            def _():
                far_copy(far_in.at[t], t, far_in, far_recv).wait_recv()

            @pl.when((t >= 1) & (t <= 2 * NP))
            def _():
                @pl.when(t - 1 >= RING)
                def _():
                    inner_copy(t - 1 - RING).wait_send()
                inner_copy(t - 1).start()

            @pl.when((g >= 1) & (g <= NP))
            def _():
                @pl.when(g - 1 >= RING)
                def _():
                    near_copy(g - 1 - RING).wait_send()
                near_copy(g - 1).start()

            for k in range(NX):
                @pl.when(g - 1 == NP + k)
                def _(k=k):
                    x_part_copy(k).start()

            @pl.when(t < 2 * NP)
            def _():
                far_in[t] = far_in[t] + part[part_index(t)]

            @pl.when((g >= 0) & (g < 2 * NP))
            def _():
                far_copy(far_in.at[g], g, side_in, side_recv).wait_recv()

                @pl.when(g < NP + NX)
                def _():
                    side_in[g] = side_in[g] + part[jnp.where(g < NP, g, g + NP - NX)]

            @pl.when(t < NP)
            def _():
                products(i)

            @pl.when(t >= 2 * NP)
            def _():
                finish(part[NP + i] + side_in[NP + NX + i] + far_in[t], first_token(z, i), i, out_store(i))

            return ()

        lax.fori_loop(0, last, step, ())
        msg_copy.wait_recv()
        msg = msg_in[...]
        for k in range(NX):
            lane = NP - NX + k
            row = msg[k + 1:k + 2]
            put(piece_m, lane, to_col(row))
            put(piece_s, lane, to_col(pltpu.roll(row, 96, 1)))
            put(piece_t, lane, to_col(pltpu.roll(row, 64, 1)))
        mine = combine(z)
        theirs = msg[0:1]
        sub, lane = iota((8, 128), 0), iota((8, 128), 1)
        tile = jnp.where(sub == 0, jnp.where(z == 1, theirs, mine),
                         jnp.where(sub == 1, jnp.where(z == 1, mine, theirs), jnp.where(lane < 32, mine, 0.0)))
        stats[2 * v + z - 1] = tile

    slot = 2 * v + z - 1

    def st_copy(slot, cross, dv):
        return pltpu.make_async_remote_copy(src_ref=stats.at[slot], dst_ref=stats.at[slot],
                                            send_sem=st_send.at[4 * cross + dv], recv_sem=st_recv.at[slot],
                                            device_id={"hid": far if cross else z, "vocab": lax.rem(v + dv, 4)},
                                            device_id_type=MESH)

    peers = [(cross, dv) for cross in (1, 0) for dv in range(4) if cross or dv]
    res_copy = pltpu.make_async_remote_copy(src_ref=res_src, dst_ref=res_in, send_sem=res_send, recv_sem=res_recv,
                                            device_id={"hid": near}, device_id_type=MESH)

    def settle(m_row, s_row, below_row):
        m_col, s_col, below = to_col(m_row), to_col(s_row), to_col(below_row)
        alive = iota((32, 128), 1) < NP
        mult = jnp.exp(jnp.where(alive, piece_m[...], m_col) - m_col)
        totals = jnp.where(alive, piece_s[...] * mult, 0.0)
        return mult / s_col, (below + (scan_lanes(totals) - totals)) / s_col

    def spread(i, src, mult, shift):
        out_ref[:, i * tok:(i + 1) * tok] = src * mult[:, i:i + 1] + shift[:, i:i + 1]

    @pl.when(inner)
    def _():
        pl.semaphore_wait(ready, 1)
        for cross, dv in peers:
            st_copy(slot, cross, dv).start()
        for k in range(RING):
            inner_copy(2 * NP - RING + k).wait_send()
            near_copy(NP - RING + k).wait_send()
        for k in range(NX):
            x_part_copy(k).wait_send()
        for other in range(8):
            @pl.when(slot != other)
            def _(other=other):
                st_copy(other, 0, 1).wait_recv()

        table = stats[...].reshape(64, 128)
        row_id = iota((64, 128), 0)
        m_row = jnp.max(table, axis=0, keepdims=True)
        scale = jnp.exp(table - m_row)
        live = (row_id & 7) < 2
        tot = jnp.where(live, pltpu.roll(table, 96, 1) * scale, 0.0)
        t_val = jnp.where(live, pltpu.roll(table, 64, 1) * scale, 0.0)
        s_row = jnp.sum(tot, axis=0, keepdims=True)

        def below(zz):
            me = v * 16 + (zz // 2) * 8 + lax.rem(zz, 2)
            return jnp.sum(jnp.where(row_id < me, tot, 0.0), axis=0, keepdims=True)

        low = (((row_id >> 3) * 2 + (row_id & 7)) * cols).astype(F32)
        tgt_lanes = jnp.sum(jnp.where(iota((32, 128), 0) == iota((32, 128), 1), tgt, 0.0), axis=0, keepdims=True)
        at_tgt = jnp.sum(jnp.where(low + float(cols) <= tgt_lanes, tot, jnp.where(low <= tgt_lanes, t_val, 0.0)),
                         axis=0, keepdims=True) / s_row
        sub = iota((8, 128), 0)
        res_src[...] = jnp.where(sub == 0, m_row, jnp.where(sub == 1, s_row, jnp.where(sub == 2, below(near), at_tgt)))
        tgt_out_ref[...] = at_tgt[:, 0:32]
        mult, shift = settle(m_row, s_row, below(z))
        res_copy.start()
        for i in range(NP - NX):
            spread(i, out_ref[:, i * tok:(i + 1) * tok], mult, shift)
        for k in range(NX):
            x_copy(k).wait_recv()
            spread(NP - NX + k, x_in[k], mult, shift)
        for cross, dv in peers:
            st_copy(slot, cross, dv).wait_send()
        res_copy.wait_send()

    @pl.when(outer)
    def _():
        res_copy.wait_recv()
        res = res_in[...]
        tgt_out_ref[...] = res[3:4, 0:32]
        mult, shift = settle(res[0:1], res[1:2], res[2:3])
        for i in range(NP):
            spread(i, out_ref[:, i * tok:(i + 1) * tok], mult, shift)
        for k in range(NX):
            x_copy(k).wait_send()


def write_kernel(table_ref, at_tgt_ref, table_hbm, at_tgt_hbm, sem, at_sem):
    copies = (pltpu.make_async_copy(table_ref, table_hbm, sem), pltpu.make_async_copy(at_tgt_ref, at_tgt_hbm, at_sem))
    for c in copies:
        c.start()
    for c in copies:
        c.wait()


def solution(mesh):
    assert mesh.shape["hid"] == 4 and mesh.shape["vocab"] == 4

    def local_step(h_blk, w_blk, temp_blk, tgt_blk):
        rows, depth = h_blk.shape
        cols = w_blk.shape[1] // 4
        tok = cols // NP
        assert rows == 32 and tok % 128 == 0
        block = (rows, tok)
        vmem, dma = pltpu.VMEM, pltpu.SemaphoreType.DMA
        hbm = pl.BlockSpec(memory_space=pltpu.MemorySpace.HBM)
        in_vmem = pl.BlockSpec(memory_space=pltpu.VMEM)
        shapes = (jax.ShapeDtypeStruct((rows, cols), F32), jax.ShapeDtypeStruct((1, rows), F32))
        table, at_tgt = pl.pallas_call(
            functools.partial(kernel, tok),
            out_shape=(pltpu.VMEM((rows, cols), F32), pltpu.VMEM((1, rows), F32)),
            in_specs=[hbm] * 4,
            out_specs=(in_vmem, in_vmem),
            scratch_shapes=[
                vmem((rows, depth), BF16), vmem((1, rows), F32), vmem((1, rows), jnp.int32),
                vmem((4 * AHEAD, depth, tok), BF16),
                vmem((4 * NP, *block), F32),
                vmem((3 * NP, *block), F32),
                vmem((2 * NP, *block), F32),
                vmem((NP, *block), F32),
                vmem((NX, *block), F32),
                vmem((NX, *block), F32),
                vmem((NX, *block), F32),
                vmem((32, 128), F32),
                vmem((32, 128), F32),
                vmem((32, 128), F32),
                vmem((8, 128), F32), vmem((8, 128), F32), vmem((8, 8, 128), F32),
                vmem((8, 128), F32), vmem((8, 128), F32),
                dma, dma, dma, dma((4 * AHEAD,)), dma((SUB,)), dma((SUB,)), dma((SUB,)),
                dma((RING,)), dma((3 * NP,)), dma((2 * NP,)),
                dma((RING,)), dma((NP,)),
                dma((NX,)), dma((NX,)), dma((NX,)), dma((NX,)),
                dma, dma, dma((8,)), dma((8,)), dma, dma, pltpu.SemaphoreType.REGULAR,
            ],
            compiler_params=pltpu.CompilerParams(collective_id=0, has_side_effects=True, vmem_limit_bytes=VMEM_LIMIT),
            name="head_cdf",
        )(h_blk, w_blk, temp_blk.reshape(1, rows), tgt_blk.reshape(1, rows))
        table, at_tgt = pl.pallas_call(
            write_kernel,
            out_shape=shapes,
            in_specs=[in_vmem, in_vmem],
            out_specs=(hbm, hbm),
            scratch_shapes=[dma, dma],
            compiler_params=pltpu.CompilerParams(vmem_limit_bytes=2 ** 20),
            name="write",
        )(table, at_tgt)
        return table, at_tgt.reshape(rows)

    return jax.shard_map(local_step, mesh=mesh,
                         in_specs=(P("data", "hid"), P("hid", "vocab"), P("data"), P("data")),
                         out_specs=(P("data", ("vocab", "hid")), P("data")), check_vma=False)
```

```python
import functools

import jax
import jax.numpy as jnp
from jax import lax
from jax.experimental import pallas as pl
from jax.experimental.pallas import tpu as pltpu
from jax.sharding import PartitionSpec as P

MESH = pl.DeviceIdType.MESH
NP = 16
NX = 6
RING = 2
LAG = 4
XSTEP = 2 * NP - 3
SUB = 3
AHEAD = 2
VMEM_LIMIT = 67043328 - 2 ** 21 - 2 ** 13
F32 = jnp.float32
BF16 = jnp.bfloat16


def iota(shape, dim):
    return lax.broadcasted_iota(jnp.int32, shape, dim)


def to_col(row):
    n = row.shape[1]
    return jnp.sum(jnp.where(iota((32, n), 0) == iota((32, n), 1), row, 0.0), axis=1, keepdims=True)


def pack_row(m, s, t):
    sub, lane = iota((32, 128), 0), iota((32, 128), 1)
    picked = jnp.where(lane == sub, m, jnp.where(lane == sub + 32, s, jnp.where(lane == sub + 64, t, 0.0)))
    return jnp.sum(picked, axis=0, keepdims=True)


def kernel(tok, h_hbm, w_hbm, temp_hbm, tgt_hbm, out_ref, tgt_out_ref,
           h_buf, temp_buf, tgt_buf, w_buf, part, far_in, side_in, near_in, x_part, x_src, x_in, piece_m, piece_s, piece_t,
           msg_src, msg_in, stats, res_src, res_in,
           h_sem, temp_sem, tgt_sem, w_sem, sub_w, sub_send, sub_recv, far_send, far_recv, side_recv, near_send, near_recv, xp_send, xp_recv, x_send, x_recv,
           msg_send, msg_recv, st_send, st_recv, res_send, res_recv, ready):
    z, v = lax.axis_index("hid"), lax.axis_index("vocab")
    outer = (z == 0) | (z == 3)
    inner = (z == 1) | (z == 2)
    far = jnp.where(z < 2, z + 1, z - 1)
    near = jnp.where(z == 1, 0, 3)
    cols = NP * tok
    last = 3 * NP - NX

    def w_load(rel, i, lane):
        slot = lax.rem(i, AHEAD) * 4 + lane
        owner = jnp.where(z < 2, rel, 3 - rel)
        start = pl.multiple_of(owner * cols + i * tok, tok)
        return pltpu.make_async_copy(w_hbm.at[:, pl.ds(start, tok)], w_buf.at[slot], w_sem.at[slot])

    h_copy = pltpu.make_async_copy(h_hbm, h_buf, h_sem)
    temp_copy = pltpu.make_async_copy(temp_hbm, temp_buf, temp_sem)
    tgt_copy = pltpu.make_async_copy(tgt_hbm, tgt_buf, tgt_sem)
    barrier = pltpu.get_barrier_semaphore()

    def greet(dev):
        pl.semaphore_signal(barrier, inc=1, device_id=dev, device_id_type=MESH)

    def part_of(k):
        at = (0, tok // 8, tok // 2, tok)
        return pl.ds(at[k], at[k + 1] - at[k])

    def sub_load(k):
        owner = jnp.where(z < 2, 3, 0)
        at = part_of(k)
        start = pl.multiple_of(owner * cols + at.start, tok // 8)
        return pltpu.make_async_copy(w_hbm.at[:, pl.ds(start, at.size)], w_buf.at[0, :, at], sub_w.at[k])

    @pl.when(inner)
    def _():
        greet({"hid": near})

    h_copy.start()
    for k in range(SUB):
        sub_load(k).start()
    greet({"hid": far})

    @pl.when(inner)
    def _():
        for dv in range(1, 4):
            greet({"vocab": lax.rem(v + dv, 4)})

    temp_copy.start()
    tgt_copy.start()

    def product(rel, i, lane):
        w_load(rel, i, lane).wait()
        part[rel * NP + i] = jnp.dot(h_buf[...], w_buf[lax.rem(i, AHEAD) * 4 + lane], preferred_element_type=F32)

        @pl.when(i + AHEAD < NP)
        def _():
            w_load(rel, i + AHEAD, lane).start()

    def products(i):
        product(0, i, 1)
        product(2, i, 2)
        product(1, i, 3)

        @pl.when(i + 1 < NP)
        def _():
            product(3, i + 1, 0)

    def sub_product(k):
        sub_load(k).wait()
        part[3 * NP, :, part_of(k)] = jnp.dot(h_buf[...], w_buf[0, :, part_of(k)], preferred_element_type=F32)

    def sub_copy(k):
        return pltpu.make_async_remote_copy(src_ref=part.at[3 * NP, :, part_of(k)], dst_ref=far_in.at[0, :, part_of(k)],
                                            send_sem=sub_send.at[k], recv_sem=sub_recv.at[k],
                                            device_id={"hid": far}, device_id_type=MESH)

    tri = (iota((128, 128), 0) <= iota((128, 128), 1)).astype(BF16)
    piece_m[...] = jnp.zeros_like(piece_m)
    piece_s[...] = jnp.zeros_like(piece_s)
    piece_t[...] = jnp.zeros_like(piece_t)

    def put(ref, lane, value):
        ref[...] = jnp.where(iota((32, 128), 1) == lane, value, ref[...])

    def finish(total, first, lane, store):
        logits = total * temp
        m = jnp.max(logits, axis=1, keepdims=True)
        e = jnp.exp(logits - m)
        n_blk = tok // 128
        terms = []
        for b in range(n_blk):
            blk = e[:, b * 128:(b + 1) * 128]
            hi = blk.astype(BF16)
            rest = blk - hi.astype(F32)
            mid = rest.astype(BF16)
            low = (rest - mid.astype(F32)).astype(BF16)
            terms += [hi, mid, low]
        sums = jnp.dot(jnp.concatenate(terms, axis=0), tri, preferred_element_type=F32)
        carry = jnp.zeros((32, 1), F32)
        hit = jnp.zeros((32, 128), F32)
        pos = tgt - first
        lanes = iota((32, 128), 1).astype(F32)
        for b in range(n_blk):
            s = sums[96 * b:96 * b + 96]
            c = (s[0:32] + s[32:64] + s[64:96]) + carry
            store(b, c)
            hit = hit + jnp.where(lanes == pos - float(b * 128), c, 0.0)
            carry = c[:, 127:128]
        put(piece_m, lane, m)
        put(piece_s, lane, carry)
        put(piece_t, lane, jnp.sum(hit, axis=1, keepdims=True))

    def first_token(owner, i):
        return (((v * 4 + owner) * NP + i) * tok).astype(F32)

    def scan_lanes(x):
        lane = iota((32, 128), 1)
        for shift in (1, 2, 4, 8):
            x = x + jnp.where(lane >= shift, pltpu.roll(x, shift, 1), 0.0)
        return x

    def combine(owner):
        lane = iota((32, 128), 1)
        live = lane < NP
        m_all, s_all, t_all = piece_m[...], piece_s[...], piece_t[...]
        m = jnp.max(jnp.where(live, m_all, m_all[:, 0:1]), axis=1, keepdims=True)
        scale = jnp.where(live, jnp.exp(jnp.where(live, m_all, m) - m), 0.0)
        tot = s_all * scale
        s = jnp.sum(tot, axis=1, keepdims=True)
        low = lane.astype(F32) * float(tok) + first_token(owner, 0)
        t = jnp.sum(jnp.where(low + float(tok) <= tgt, tot, jnp.where(low <= tgt, t_all * scale, 0.0)),
                    axis=1, keepdims=True)
        return pack_row(m, s, t)

    def far_copy(src, t, dst, sems):
        return pltpu.make_async_remote_copy(src_ref=src, dst_ref=dst.at[t], send_sem=far_send.at[lax.rem(t, RING)],
                                            recv_sem=sems.at[t], device_id={"hid": far}, device_id_type=MESH)

    def part_index(t):
        i, ph = lax.rem(t, NP), t // NP
        return (3 - ph) * NP + jnp.where(ph == 1, lax.rem(i + NP - NX, NP), i)

    def outer_copy(t):
        return far_copy(part.at[part_index(t)], t, far_in, far_recv)

    def inner_copy(t):
        return far_copy(far_in.at[t], t, side_in, side_recv)

    def near_copy(g):
        return pltpu.make_async_remote_copy(src_ref=side_in.at[g], dst_ref=near_in.at[g],
                                            send_sem=near_send.at[lax.rem(g, RING)], recv_sem=near_recv.at[g],
                                            device_id={"hid": near}, device_id_type=MESH)

    def x_part_copy(k):
        return pltpu.make_async_remote_copy(src_ref=side_in.at[NP + k], dst_ref=x_part.at[k],
                                            send_sem=xp_send.at[k], recv_sem=xp_recv.at[k],
                                            device_id={"hid": near}, device_id_type=MESH)

    def x_copy(k):
        return pltpu.make_async_remote_copy(src_ref=x_src.at[k], dst_ref=x_in.at[k], send_sem=x_send.at[k],
                                            recv_sem=x_recv.at[k], device_id={"hid": far}, device_id_type=MESH)

    msg_copy = pltpu.make_async_remote_copy(src_ref=msg_src, dst_ref=msg_in, send_sem=msg_send, recv_sem=msg_recv,
                                            device_id={"hid": far}, device_id_type=MESH)

    @pl.when(inner)
    def _():
        for k in range(SUB):
            sub_copy(k).wait_recv()

    h_copy.wait()
    for k in range(SUB):
        sub_product(k)
        if k == 0:
            for i in range(AHEAD):
                for lane, rel in ((0, 3), (1, 0), (2, 2), (3, 1)):
                    if i or lane:
                        w_load(rel, i, lane).start()

            @pl.when(outer)
            def _():
                pl.semaphore_wait(barrier, 1)

        @pl.when(outer)
        def _(k=k):
            sub_copy(k).start()

    w_load(3, AHEAD, 0).start()
    temp_copy.wait()
    tgt_copy.wait()
    temp = to_col(temp_buf[...])
    tgt = to_col(tgt_buf[...].astype(F32))

    @pl.when(inner)
    def _():
        pl.semaphore_wait(barrier, 5)
        pl.semaphore_signal(ready, inc=1, device_id={"hid": far}, device_id_type=MESH)

    def out_store(i):
        def store(b, c):
            out_ref[:, pl.ds(pl.multiple_of(i * tok + b * 128, 128), 128)] = c
        return store

    @pl.when(outer)
    def _():
        def step(t, _):
            i = lax.rem(t, NP)

            @pl.when(t > RING)
            def _():
                outer_copy(t - RING).wait_send()

            @pl.when(t > 0)
            def _():
                outer_copy(t).start()

            @pl.when(t == 0)
            def _():
                sub_copy(1).wait_send()

            @pl.when(t < NP)
            def _():
                products(i)

            @pl.when((t >= NP) & (t < 2 * NP))
            def _():
                near_copy(i).wait_recv()
                finish(part[i] + near_in[i], first_token(z, i), i, out_store(i))

            @pl.when((t >= XSTEP) & (t < XSTEP + NX))
            def _():
                k = t - XSTEP

                def store(b, c):
                    x_src[k, :, b * 128:(b + 1) * 128] = c
                x_part_copy(k).wait_recv()
                finish(part[2 * NP - NX + k] + x_part[k], first_token(far, NP - NX + k), NP + k, store)

            @pl.when(t == XSTEP + NX)
            def _():
                sub = iota((8, 128), 0)
                tile = jnp.where(sub == 0, combine(z), 0.0)
                for k in range(NX):
                    lane = NP + k
                    row = pack_row(piece_m[:, lane:lane + 1], piece_s[:, lane:lane + 1], piece_t[:, lane:lane + 1])
                    tile = jnp.where(sub == k + 1, row, tile)
                msg_src[...] = tile

            @pl.when(t == XSTEP + NX + 1)
            def _():
                msg_copy.start()

            return ()

        lax.fori_loop(0, last, step, ())
        for k in range(NX):
            x_copy(k).start()
        for k in (0, 2):
            sub_copy(k).wait_send()
        for k in range(RING):
            outer_copy(last - RING + k).wait_send()
        msg_copy.wait_send()

    @pl.when(inner)
    def _():
        def step(t, _):
            i = lax.rem(t, NP)
            g = t - LAG

            @pl.when(t > 0)
            def _():
                far_copy(far_in.at[t], t, far_in, far_recv).wait_recv()

            @pl.when((t >= 1) & (t <= 2 * NP))
            def _():
                @pl.when(t - 1 >= RING)
                def _():
                    inner_copy(t - 1 - RING).wait_send()
                inner_copy(t - 1).start()

            @pl.when((g >= 1) & (g <= NP))
            def _():
                @pl.when(g - 1 >= RING)
                def _():
                    near_copy(g - 1 - RING).wait_send()
                near_copy(g - 1).start()

            for k in range(NX):
                @pl.when(g - 1 == NP + k)
                def _(k=k):
                    x_part_copy(k).start()

            @pl.when(t < 2 * NP)
            def _():
                far_in[t] = far_in[t] + part[part_index(t)]

            @pl.when((g >= 0) & (g < 2 * NP))
            def _():
                far_copy(far_in.at[g], g, side_in, side_recv).wait_recv()

                @pl.when(g < NP + NX)
                def _():
                    side_in[g] = side_in[g] + part[jnp.where(g < NP, g, g + NP - NX)]

            @pl.when(t < NP)
            def _():
                products(i)

            @pl.when(t >= 2 * NP)
            def _():
                finish(part[NP + i] + side_in[NP + NX + i] + far_in[t], first_token(z, i), i, out_store(i))

            return ()

        lax.fori_loop(0, last, step, ())
        msg_copy.wait_recv()
        msg = msg_in[...]
        for k in range(NX):
            lane = NP - NX + k
            row = msg[k + 1:k + 2]
            put(piece_m, lane, to_col(row))
            put(piece_s, lane, to_col(pltpu.roll(row, 96, 1)))
            put(piece_t, lane, to_col(pltpu.roll(row, 64, 1)))
        mine = combine(z)
        theirs = msg[0:1]
        sub, lane = iota((8, 128), 0), iota((8, 128), 1)
        tile = jnp.where(sub == 0, jnp.where(z == 1, theirs, mine),
                         jnp.where(sub == 1, jnp.where(z == 1, mine, theirs), jnp.where(lane < 32, mine, 0.0)))
        stats[2 * v + z - 1] = tile

    slot = 2 * v + z - 1

    def st_copy(slot, cross, dv):
        return pltpu.make_async_remote_copy(src_ref=stats.at[slot], dst_ref=stats.at[slot],
                                            send_sem=st_send.at[4 * cross + dv], recv_sem=st_recv.at[slot],
                                            device_id={"hid": far if cross else z, "vocab": lax.rem(v + dv, 4)},
                                            device_id_type=MESH)

    peers = [(cross, dv) for cross in (1, 0) for dv in range(4) if cross or dv]
    res_copy = pltpu.make_async_remote_copy(src_ref=res_src, dst_ref=res_in, send_sem=res_send, recv_sem=res_recv,
                                            device_id={"hid": near}, device_id_type=MESH)

    def settle(m_row, s_row, below_row):
        m_col, s_col, below = to_col(m_row), to_col(s_row), to_col(below_row)
        alive = iota((32, 128), 1) < NP
        mult = jnp.exp(jnp.where(alive, piece_m[...], m_col) - m_col)
        totals = jnp.where(alive, piece_s[...] * mult, 0.0)
        return mult / s_col, (below + (scan_lanes(totals) - totals)) / s_col

    def spread(i, src, mult, shift):
        out_ref[:, i * tok:(i + 1) * tok] = src * mult[:, i:i + 1] + shift[:, i:i + 1]

    @pl.when(inner)
    def _():
        pl.semaphore_wait(ready, 1)
        for cross, dv in peers:
            st_copy(slot, cross, dv).start()
        for k in range(RING):
            inner_copy(2 * NP - RING + k).wait_send()
            near_copy(NP - RING + k).wait_send()
        for k in range(NX):
            x_part_copy(k).wait_send()
        for other in range(8):
            @pl.when(slot != other)
            def _(other=other):
                st_copy(other, 0, 1).wait_recv()

        table = stats[...].reshape(64, 128)
        row_id = iota((64, 128), 0)
        m_row = jnp.max(table, axis=0, keepdims=True)
        scale = jnp.exp(table - m_row)
        live = (row_id & 7) < 2
        tot = jnp.where(live, pltpu.roll(table, 96, 1) * scale, 0.0)
        t_val = jnp.where(live, pltpu.roll(table, 64, 1) * scale, 0.0)
        s_row = jnp.sum(tot, axis=0, keepdims=True)

        def below(zz):
            me = v * 16 + (zz // 2) * 8 + lax.rem(zz, 2)
            return jnp.sum(jnp.where(row_id < me, tot, 0.0), axis=0, keepdims=True)

        low = (((row_id >> 3) * 2 + (row_id & 7)) * cols).astype(F32)
        tgt_lanes = jnp.sum(jnp.where(iota((32, 128), 0) == iota((32, 128), 1), tgt, 0.0), axis=0, keepdims=True)
        at_tgt = jnp.sum(jnp.where(low + float(cols) <= tgt_lanes, tot, jnp.where(low <= tgt_lanes, t_val, 0.0)),
                         axis=0, keepdims=True) / s_row
        sub = iota((8, 128), 0)
        res_src[...] = jnp.where(sub == 0, m_row, jnp.where(sub == 1, s_row, jnp.where(sub == 2, below(near), at_tgt)))
        tgt_out_ref[...] = at_tgt[:, 0:32]
        mult, shift = settle(m_row, s_row, below(z))
        res_copy.start()
        for i in range(NP - NX):
            spread(i, out_ref[:, i * tok:(i + 1) * tok], mult, shift)
        for cross, dv in peers:
            st_copy(slot, cross, dv).wait_send()
        res_copy.wait_send()
        for k in range(NX):
            x_copy(k).wait_recv()
            spread(NP - NX + k, x_in[k], mult, shift)

    @pl.when(outer)
    def _():
        res_copy.wait_recv()
        res = res_in[...]
        tgt_out_ref[...] = res[3:4, 0:32]
        mult, shift = settle(res[0:1], res[1:2], res[2:3])
        for i in range(NP):
            spread(i, out_ref[:, i * tok:(i + 1) * tok], mult, shift)
        for k in range(NX):
            x_copy(k).wait_send()


def write_kernel(table_ref, at_tgt_ref, table_hbm, at_tgt_hbm, sem, at_sem):
    copies = (pltpu.make_async_copy(table_ref, table_hbm, sem), pltpu.make_async_copy(at_tgt_ref, at_tgt_hbm, at_sem))
    for c in copies:
        c.start()
    for c in copies:
        c.wait()


def solution(mesh):
    assert mesh.shape["hid"] == 4 and mesh.shape["vocab"] == 4

    def local_step(h_blk, w_blk, temp_blk, tgt_blk):
        rows, depth = h_blk.shape
        cols = w_blk.shape[1] // 4
        tok = cols // NP
        assert rows == 32 and tok % 128 == 0
        block = (rows, tok)
        vmem, dma = pltpu.VMEM, pltpu.SemaphoreType.DMA
        hbm = pl.BlockSpec(memory_space=pltpu.MemorySpace.HBM)
        in_vmem = pl.BlockSpec(memory_space=pltpu.VMEM)
        shapes = (jax.ShapeDtypeStruct((rows, cols), F32), jax.ShapeDtypeStruct((1, rows), F32))
        table, at_tgt = pl.pallas_call(
            functools.partial(kernel, tok),
            out_shape=(pltpu.VMEM((rows, cols), F32), pltpu.VMEM((1, rows), F32)),
            in_specs=[hbm] * 4,
            out_specs=(in_vmem, in_vmem),
            scratch_shapes=[
                vmem((rows, depth), BF16), vmem((1, rows), F32), vmem((1, rows), jnp.int32),
                vmem((4 * AHEAD, depth, tok), BF16),
                vmem((4 * NP, *block), F32),
                vmem((3 * NP, *block), F32),
                vmem((2 * NP, *block), F32),
                vmem((NP, *block), F32),
                vmem((NX, *block), F32),
                vmem((NX, *block), F32),
                vmem((NX, *block), F32),
                vmem((32, 128), F32),
                vmem((32, 128), F32),
                vmem((32, 128), F32),
                vmem((8, 128), F32), vmem((8, 128), F32), vmem((8, 8, 128), F32),
                vmem((8, 128), F32), vmem((8, 128), F32),
                dma, dma, dma, dma((4 * AHEAD,)), dma((SUB,)), dma((SUB,)), dma((SUB,)),
                dma((RING,)), dma((3 * NP,)), dma((2 * NP,)),
                dma((RING,)), dma((NP,)),
                dma((NX,)), dma((NX,)), dma((NX,)), dma((NX,)),
                dma, dma, dma((8,)), dma((8,)), dma, dma, pltpu.SemaphoreType.REGULAR,
            ],
            compiler_params=pltpu.CompilerParams(collective_id=0, has_side_effects=True, vmem_limit_bytes=VMEM_LIMIT),
            name="head_cdf",
        )(h_blk, w_blk, temp_blk.reshape(1, rows), tgt_blk.reshape(1, rows))
        table, at_tgt = pl.pallas_call(
            write_kernel,
            out_shape=shapes,
            in_specs=[in_vmem, in_vmem],
            out_specs=(hbm, hbm),
            scratch_shapes=[dma, dma],
            compiler_params=pltpu.CompilerParams(vmem_limit_bytes=2 ** 20),
            name="write",
        )(table, at_tgt)
        return table, at_tgt.reshape(rows)

    return jax.shard_map(local_step, mesh=mesh,
                         in_specs=(P("data", "hid"), P("hid", "vocab"), P("data"), P("data")),
                         out_specs=(P("data", ("vocab", "hid")), P("data")), check_vma=False)
```

```python
import functools

import jax
import jax.numpy as jnp
from jax import lax
from jax.experimental import pallas as pl
from jax.experimental.pallas import tpu as pltpu
from jax.sharding import PartitionSpec as P

MESH = pl.DeviceIdType.MESH
NP = 16
NX = 6
RING = 2
LAG = 4
XSTEP = 2 * NP - 3
SUB = 3
X_SENDS = ((0, 2), (2, 3), (5, 1))
AHEAD = 2
VMEM_LIMIT = 67043328 - 2 ** 21 - 2 ** 13
F32 = jnp.float32
BF16 = jnp.bfloat16


def iota(shape, dim):
    return lax.broadcasted_iota(jnp.int32, shape, dim)


def to_col(row):
    n = row.shape[1]
    return jnp.sum(jnp.where(iota((32, n), 0) == iota((32, n), 1), row, 0.0), axis=1, keepdims=True)


def pack_row(m, s, t):
    sub, lane = iota((32, 128), 0), iota((32, 128), 1)
    picked = jnp.where(lane == sub, m, jnp.where(lane == sub + 32, s, jnp.where(lane == sub + 64, t, 0.0)))
    return jnp.sum(picked, axis=0, keepdims=True)


def kernel(tok, h_hbm, w_hbm, temp_hbm, tgt_hbm, out_ref, tgt_out_ref,
           h_buf, temp_buf, tgt_buf, w_buf, part, far_in, side_in, near_in, x_part, x_src, x_in, piece_m, piece_s, piece_t,
           msg_src, msg_in, stats, res_src, res_in,
           h_sem, temp_sem, tgt_sem, w_sem, sub_w, sub_send, sub_recv, far_send, far_recv, side_recv, near_send, near_recv, xp_send, xp_recv, x_send, x_recv,
           msg_send, msg_recv, st_send, st_recv, res_send, res_recv, ready):
    z, v = lax.axis_index("hid"), lax.axis_index("vocab")
    outer = (z == 0) | (z == 3)
    inner = (z == 1) | (z == 2)
    far = jnp.where(z < 2, z + 1, z - 1)
    near = jnp.where(z == 1, 0, 3)
    cols = NP * tok
    last = 3 * NP - NX

    def w_load(rel, i, lane):
        slot = lax.rem(i, AHEAD) * 4 + lane
        owner = jnp.where(z < 2, rel, 3 - rel)
        start = pl.multiple_of(owner * cols + i * tok, tok)
        return pltpu.make_async_copy(w_hbm.at[:, pl.ds(start, tok)], w_buf.at[slot], w_sem.at[slot])

    h_copy = pltpu.make_async_copy(h_hbm, h_buf, h_sem)
    temp_copy = pltpu.make_async_copy(temp_hbm, temp_buf, temp_sem)
    tgt_copy = pltpu.make_async_copy(tgt_hbm, tgt_buf, tgt_sem)
    barrier = pltpu.get_barrier_semaphore()

    def greet(dev):
        pl.semaphore_signal(barrier, inc=1, device_id=dev, device_id_type=MESH)

    def part_of(k):
        at = (0, tok // 8, tok // 2, tok)
        return pl.ds(at[k], at[k + 1] - at[k])

    def sub_load(k):
        owner = jnp.where(z < 2, 3, 0)
        at = part_of(k)
        start = pl.multiple_of(owner * cols + at.start, tok // 8)
        return pltpu.make_async_copy(w_hbm.at[:, pl.ds(start, at.size)], w_buf.at[0, :, at], sub_w.at[k])

    @pl.when(inner)
    def _():
        greet({"hid": near})

    h_copy.start()
    for k in range(SUB):
        sub_load(k).start()
    greet({"hid": far})

    @pl.when(inner)
    def _():
        for dv in range(1, 4):
            greet({"vocab": lax.rem(v + dv, 4)})

    temp_copy.start()
    tgt_copy.start()

    def product(rel, i, lane):
        w_load(rel, i, lane).wait()
        part[rel * NP + i] = jnp.dot(h_buf[...], w_buf[lax.rem(i, AHEAD) * 4 + lane], preferred_element_type=F32)

        @pl.when(i + AHEAD < NP)
        def _():
            w_load(rel, i + AHEAD, lane).start()

    def products(i):
        product(0, i, 1)
        product(2, i, 2)
        product(1, i, 3)

        @pl.when(i + 2 < NP)
        def _():
            product(3, i + 2, 0)

    def sub_product(k):
        sub_load(k).wait()
        part[3 * NP, :, part_of(k)] = jnp.dot(h_buf[...], w_buf[0, :, part_of(k)], preferred_element_type=F32)

    def sub_copy(k):
        src, dst = part.at[3 * NP + 1], far_in.at[1]
        if k < SUB:
            src, dst = part.at[3 * NP, :, part_of(k)], far_in.at[0, :, part_of(k)]
        return pltpu.make_async_remote_copy(src_ref=src, dst_ref=dst,
                                            send_sem=sub_send.at[k], recv_sem=sub_recv.at[k],
                                            device_id={"hid": far}, device_id_type=MESH)

    tri = (iota((128, 128), 0) <= iota((128, 128), 1)).astype(BF16)
    piece_m[...] = jnp.zeros_like(piece_m)
    piece_s[...] = jnp.zeros_like(piece_s)
    piece_t[...] = jnp.zeros_like(piece_t)

    def put(ref, lane, value):
        ref[...] = jnp.where(iota((32, 128), 1) == lane, value, ref[...])

    def finish(total, first, lane, store):
        logits = total * temp
        m = jnp.max(logits, axis=1, keepdims=True)
        e = jnp.exp(logits - m)
        n_blk = tok // 128
        terms = []
        for b in range(n_blk):
            blk = e[:, b * 128:(b + 1) * 128]
            hi = blk.astype(BF16)
            rest = blk - hi.astype(F32)
            mid = rest.astype(BF16)
            low = (rest - mid.astype(F32)).astype(BF16)
            terms += [hi, mid, low]
        sums = jnp.dot(jnp.concatenate(terms, axis=0), tri, preferred_element_type=F32)
        carry = jnp.zeros((32, 1), F32)
        hit = jnp.zeros((32, 128), F32)
        pos = tgt - first
        lanes = iota((32, 128), 1).astype(F32)
        for b in range(n_blk):
            s = sums[96 * b:96 * b + 96]
            c = (s[0:32] + s[32:64] + s[64:96]) + carry
            store(b, c)
            hit = hit + jnp.where(lanes == pos - float(b * 128), c, 0.0)
            carry = c[:, 127:128]
        put(piece_m, lane, m)
        put(piece_s, lane, carry)
        put(piece_t, lane, jnp.sum(hit, axis=1, keepdims=True))

    def first_token(owner, i):
        return (((v * 4 + owner) * NP + i) * tok).astype(F32)

    def scan_lanes(x):
        lane = iota((32, 128), 1)
        for shift in (1, 2, 4, 8):
            x = x + jnp.where(lane >= shift, pltpu.roll(x, shift, 1), 0.0)
        return x

    def combine(owner):
        lane = iota((32, 128), 1)
        live = lane < NP
        m_all, s_all, t_all = piece_m[...], piece_s[...], piece_t[...]
        m = jnp.max(jnp.where(live, m_all, m_all[:, 0:1]), axis=1, keepdims=True)
        scale = jnp.where(live, jnp.exp(jnp.where(live, m_all, m) - m), 0.0)
        tot = s_all * scale
        s = jnp.sum(tot, axis=1, keepdims=True)
        low = lane.astype(F32) * float(tok) + first_token(owner, 0)
        t = jnp.sum(jnp.where(low + float(tok) <= tgt, tot, jnp.where(low <= tgt, t_all * scale, 0.0)),
                    axis=1, keepdims=True)
        return pack_row(m, s, t)

    def far_copy(src, t, dst, sems):
        return pltpu.make_async_remote_copy(src_ref=src, dst_ref=dst.at[t], send_sem=far_send.at[lax.rem(t, RING)],
                                            recv_sem=sems.at[t], device_id={"hid": far}, device_id_type=MESH)

    def part_index(t):
        i, ph = lax.rem(t, NP), t // NP
        return (3 - ph) * NP + jnp.where(ph == 1, lax.rem(i + NP - NX, NP), i)

    def outer_copy(u):
        return pltpu.make_async_remote_copy(src_ref=part.at[pl.ds(part_index(2 * u), 2)], dst_ref=far_in.at[pl.ds(2 * u, 2)],
                                            send_sem=far_send.at[lax.rem(u, RING)], recv_sem=far_recv.at[u],
                                            device_id={"hid": far}, device_id_type=MESH)

    def inner_copy(t):
        return far_copy(far_in.at[t], t, side_in, side_recv)

    def near_copy(g):
        return pltpu.make_async_remote_copy(src_ref=side_in.at[g], dst_ref=near_in.at[g],
                                            send_sem=near_send.at[lax.rem(g, RING)], recv_sem=near_recv.at[g],
                                            device_id={"hid": near}, device_id_type=MESH)

    def x_part_copy(k):
        return pltpu.make_async_remote_copy(src_ref=side_in.at[NP + k], dst_ref=x_part.at[k],
                                            send_sem=xp_send.at[k], recv_sem=xp_recv.at[k],
                                            device_id={"hid": near}, device_id_type=MESH)

    def x_copy(j):
        at = pl.ds(*X_SENDS[j])
        return pltpu.make_async_remote_copy(src_ref=x_src.at[at], dst_ref=x_in.at[at], send_sem=x_send.at[j],
                                            recv_sem=x_recv.at[j], device_id={"hid": far}, device_id_type=MESH)

    msg_copy = pltpu.make_async_remote_copy(src_ref=msg_src, dst_ref=msg_in, send_sem=msg_send, recv_sem=msg_recv,
                                            device_id={"hid": far}, device_id_type=MESH)

    @pl.when(inner)
    def _():
        for k in range(SUB):
            sub_copy(k).wait_recv()

    h_copy.wait()
    for k in range(SUB):
        sub_product(k)
        if k == 0:
            for i in range(AHEAD):
                for lane, rel in ((0, 3), (1, 0), (2, 2), (3, 1)):
                    j = 1 - i if lane == 0 else i
                    if j or lane:
                        w_load(rel, j, lane).start()

            @pl.when(outer)
            def _():
                pl.semaphore_wait(barrier, 1)

        @pl.when(outer)
        def _(k=k):
            sub_copy(k).start()

    w_load(3, AHEAD, 0).start()
    product(3, 1, 0)

    @pl.when(outer)
    def _():
        sub_copy(SUB).start()

    temp_copy.wait()
    tgt_copy.wait()
    temp = to_col(temp_buf[...])
    tgt = to_col(tgt_buf[...].astype(F32))

    @pl.when(inner)
    def _():
        pl.semaphore_wait(barrier, 5)
        pl.semaphore_signal(ready, inc=1, device_id={"hid": far}, device_id_type=MESH)

    def out_store(i):
        def store(b, c):
            out_ref[:, pl.ds(pl.multiple_of(i * tok + b * 128, 128), 128)] = c
        return store

    @pl.when(outer)
    def _():
        def step(t, _):
            i = lax.rem(t, NP)

            u = t // 2

            @pl.when((t > 2 * RING) & (lax.rem(t, 2) == 0))
            def _():
                outer_copy(u - RING).wait_send()

            @pl.when((t > 0) & (lax.rem(t, 2) == 0))
            def _():
                outer_copy(u).start()

            @pl.when(t == 0)
            def _():
                sub_copy(1).wait_send()

            @pl.when(t < NP)
            def _():
                products(i)

            @pl.when((t >= NP) & (t < 2 * NP))
            def _():
                near_copy(i).wait_recv()
                finish(part[i] + near_in[i], first_token(z, i), i, out_store(i))

            @pl.when((t >= XSTEP) & (t < XSTEP + NX))
            def _():
                k = t - XSTEP

                def store(b, c):
                    x_src[k, :, b * 128:(b + 1) * 128] = c
                x_part_copy(k).wait_recv()
                finish(part[2 * NP - NX + k] + x_part[k], first_token(far, NP - NX + k), NP + k, store)

            @pl.when(t == XSTEP + NX)
            def _():
                sub = iota((8, 128), 0)
                tile = jnp.where(sub == 0, combine(z), 0.0)
                for k in range(NX):
                    lane = NP + k
                    row = pack_row(piece_m[:, lane:lane + 1], piece_s[:, lane:lane + 1], piece_t[:, lane:lane + 1])
                    tile = jnp.where(sub == k + 1, row, tile)
                msg_src[...] = tile

            @pl.when(t == XSTEP + NX + 1)
            def _():
                msg_copy.start()

            return ()

        lax.fori_loop(0, last, step, ())
        for j in range(len(X_SENDS)):
            x_copy(j).start()
        for k in (0, *range(2, SUB + 1)):
            sub_copy(k).wait_send()
        for k in range(RING):
            outer_copy(last // 2 - RING + k).wait_send()
        msg_copy.wait_send()

    @pl.when(inner)
    def _():
        def step(t, _):
            i = lax.rem(t, NP)
            g = t - LAG

            @pl.when(t == 1)
            def _():
                sub_copy(SUB).wait_recv()

            @pl.when((t > 1) & (lax.rem(t, 2) == 0))
            def _():
                outer_copy(t // 2).wait_recv()

            @pl.when((t >= 1) & (t <= 2 * NP))
            def _():
                @pl.when(t - 1 >= RING)
                def _():
                    inner_copy(t - 1 - RING).wait_send()
                inner_copy(t - 1).start()

            @pl.when((g >= 1) & (g <= NP))
            def _():
                @pl.when(g - 1 >= RING)
                def _():
                    near_copy(g - 1 - RING).wait_send()
                near_copy(g - 1).start()

            for k in range(NX):
                @pl.when(g - 1 == NP + k)
                def _(k=k):
                    x_part_copy(k).start()

            @pl.when(t < 2 * NP)
            def _():
                far_in[t] = far_in[t] + part[part_index(t)]

            @pl.when((g >= 0) & (g < 2 * NP))
            def _():
                far_copy(far_in.at[g], g, side_in, side_recv).wait_recv()

                @pl.when(g < NP + NX)
                def _():
                    side_in[g] = side_in[g] + part[jnp.where(g < NP, g, g + NP - NX)]

            @pl.when(t < NP)
            def _():
                products(i)

            @pl.when(t >= 2 * NP)
            def _():
                finish(part[NP + i] + side_in[NP + NX + i] + far_in[t], first_token(z, i), i, out_store(i))

            return ()

        lax.fori_loop(0, last, step, ())
        msg_copy.wait_recv()
        msg = msg_in[...]
        for k in range(NX):
            lane = NP - NX + k
            row = msg[k + 1:k + 2]
            put(piece_m, lane, to_col(row))
            put(piece_s, lane, to_col(pltpu.roll(row, 96, 1)))
            put(piece_t, lane, to_col(pltpu.roll(row, 64, 1)))
        mine = combine(z)
        theirs = msg[0:1]
        sub, lane = iota((8, 128), 0), iota((8, 128), 1)
        tile = jnp.where(sub == 0, jnp.where(z == 1, theirs, mine),
                         jnp.where(sub == 1, jnp.where(z == 1, mine, theirs), jnp.where(lane < 32, mine, 0.0)))
        stats[2 * v + z - 1] = tile

    slot = 2 * v + z - 1

    def st_copy(slot, cross, dv):
        return pltpu.make_async_remote_copy(src_ref=stats.at[slot], dst_ref=stats.at[slot],
                                            send_sem=st_send.at[4 * cross + dv], recv_sem=st_recv.at[slot],
                                            device_id={"hid": far if cross else z, "vocab": lax.rem(v + dv, 4)},
                                            device_id_type=MESH)

    peers = [(cross, dv) for cross in (1, 0) for dv in range(4) if cross or dv]
    res_copy = pltpu.make_async_remote_copy(src_ref=res_src, dst_ref=res_in, send_sem=res_send, recv_sem=res_recv,
                                            device_id={"hid": near}, device_id_type=MESH)

    def settle(m_row, s_row, below_row):
        m_col, s_col, below = to_col(m_row), to_col(s_row), to_col(below_row)
        alive = iota((32, 128), 1) < NP
        mult = jnp.exp(jnp.where(alive, piece_m[...], m_col) - m_col)
        totals = jnp.where(alive, piece_s[...] * mult, 0.0)
        return mult / s_col, (below + (scan_lanes(totals) - totals)) / s_col

    def spread(i, src, mult, shift):
        out_ref[:, i * tok:(i + 1) * tok] = src * mult[:, i:i + 1] + shift[:, i:i + 1]

    @pl.when(inner)
    def _():
        pl.semaphore_wait(ready, 1)
        for cross, dv in peers:
            st_copy(slot, cross, dv).start()
        for k in range(RING):
            inner_copy(2 * NP - RING + k).wait_send()
            near_copy(NP - RING + k).wait_send()
        for k in range(NX):
            x_part_copy(k).wait_send()
        for other in range(8):
            @pl.when(slot != other)
            def _(other=other):
                st_copy(other, 0, 1).wait_recv()

        table = stats[...].reshape(64, 128)
        row_id = iota((64, 128), 0)
        m_row = jnp.max(table, axis=0, keepdims=True)
        scale = jnp.exp(table - m_row)
        live = (row_id & 7) < 2
        tot = jnp.where(live, pltpu.roll(table, 96, 1) * scale, 0.0)
        t_val = jnp.where(live, pltpu.roll(table, 64, 1) * scale, 0.0)
        s_row = jnp.sum(tot, axis=0, keepdims=True)

        def below(zz):
            me = v * 16 + (zz // 2) * 8 + lax.rem(zz, 2)
            return jnp.sum(jnp.where(row_id < me, tot, 0.0), axis=0, keepdims=True)

        low = (((row_id >> 3) * 2 + (row_id & 7)) * cols).astype(F32)
        tgt_lanes = jnp.sum(jnp.where(iota((32, 128), 0) == iota((32, 128), 1), tgt, 0.0), axis=0, keepdims=True)
        at_tgt = jnp.sum(jnp.where(low + float(cols) <= tgt_lanes, tot, jnp.where(low <= tgt_lanes, t_val, 0.0)),
                         axis=0, keepdims=True) / s_row
        sub = iota((8, 128), 0)
        res_src[...] = jnp.where(sub == 0, m_row, jnp.where(sub == 1, s_row, jnp.where(sub == 2, below(near), at_tgt)))
        tgt_out_ref[...] = at_tgt[:, 0:32]
        mult, shift = settle(m_row, s_row, below(z))
        res_copy.start()
        for i in range(NP - NX):
            spread(i, out_ref[:, i * tok:(i + 1) * tok], mult, shift)
        for cross, dv in peers:
            st_copy(slot, cross, dv).wait_send()
        res_copy.wait_send()
        for j, (first, count) in enumerate(X_SENDS):
            x_copy(j).wait_recv()
            for k in range(first, first + count):
                spread(NP - NX + k, x_in[k], mult, shift)

    @pl.when(outer)
    def _():
        res_copy.wait_recv()
        res = res_in[...]
        tgt_out_ref[...] = res[3:4, 0:32]
        mult, shift = settle(res[0:1], res[1:2], res[2:3])
        for i in range(NP):
            spread(i, out_ref[:, i * tok:(i + 1) * tok], mult, shift)
        for j in range(len(X_SENDS)):
            x_copy(j).wait_send()


def write_kernel(table_ref, at_tgt_ref, table_hbm, at_tgt_hbm, sem, at_sem):
    copies = (pltpu.make_async_copy(table_ref, table_hbm, sem), pltpu.make_async_copy(at_tgt_ref, at_tgt_hbm, at_sem))
    for c in copies:
        c.start()
    for c in copies:
        c.wait()


def solution(mesh):
    assert mesh.shape["hid"] == 4 and mesh.shape["vocab"] == 4

    def local_step(h_blk, w_blk, temp_blk, tgt_blk):
        rows, depth = h_blk.shape
        cols = w_blk.shape[1] // 4
        tok = cols // NP
        assert rows == 32 and tok % 128 == 0
        block = (rows, tok)
        vmem, dma = pltpu.VMEM, pltpu.SemaphoreType.DMA
        hbm = pl.BlockSpec(memory_space=pltpu.MemorySpace.HBM)
        in_vmem = pl.BlockSpec(memory_space=pltpu.VMEM)
        shapes = (jax.ShapeDtypeStruct((rows, cols), F32), jax.ShapeDtypeStruct((1, rows), F32))
        table, at_tgt = pl.pallas_call(
            functools.partial(kernel, tok),
            out_shape=(pltpu.VMEM((rows, cols), F32), pltpu.VMEM((1, rows), F32)),
            in_specs=[hbm] * 4,
            out_specs=(in_vmem, in_vmem),
            scratch_shapes=[
                vmem((rows, depth), BF16), vmem((1, rows), F32), vmem((1, rows), jnp.int32),
                vmem((4 * AHEAD, depth, tok), BF16),
                vmem((4 * NP, *block), F32),
                vmem((3 * NP, *block), F32),
                vmem((2 * NP, *block), F32),
                vmem((NP, *block), F32),
                vmem((NX, *block), F32),
                vmem((NX, *block), F32),
                vmem((NX, *block), F32),
                vmem((32, 128), F32),
                vmem((32, 128), F32),
                vmem((32, 128), F32),
                vmem((8, 128), F32), vmem((8, 128), F32), vmem((8, 8, 128), F32),
                vmem((8, 128), F32), vmem((8, 128), F32),
                dma, dma, dma, dma((4 * AHEAD,)), dma((SUB,)), dma((SUB + 1,)), dma((SUB + 1,)),
                dma((RING,)), dma((3 * NP // 2,)), dma((2 * NP,)),
                dma((RING,)), dma((NP,)),
                dma((NX,)), dma((NX,)), dma((len(X_SENDS),)), dma((len(X_SENDS),)),
                dma, dma, dma((8,)), dma((8,)), dma, dma, pltpu.SemaphoreType.REGULAR,
            ],
            compiler_params=pltpu.CompilerParams(collective_id=0, has_side_effects=True, vmem_limit_bytes=VMEM_LIMIT),
            name="head_cdf",
        )(h_blk, w_blk, temp_blk.reshape(1, rows), tgt_blk.reshape(1, rows))
        table, at_tgt = pl.pallas_call(
            write_kernel,
            out_shape=shapes,
            in_specs=[in_vmem, in_vmem],
            out_specs=(hbm, hbm),
            scratch_shapes=[dma, dma],
            compiler_params=pltpu.CompilerParams(vmem_limit_bytes=2 ** 20),
            name="write",
        )(table, at_tgt)
        return table, at_tgt.reshape(rows)

    return jax.shard_map(local_step, mesh=mesh,
                         in_specs=(P("data", "hid"), P("hid", "vocab"), P("data"), P("data")),
                         out_specs=(P("data", ("vocab", "hid")), P("data")), check_vma=False)
```

```python
import functools

import jax
import jax.numpy as jnp
from jax import lax
from jax.experimental import pallas as pl
from jax.experimental.pallas import tpu as pltpu
from jax.sharding import PartitionSpec as P

MESH = pl.DeviceIdType.MESH
NP = 16
NX = 6
RING = 2
LAG = 4
XSTEP = 2 * NP - 3
SUB = 3
SENDS = (*((t, 2) for t in range(2, NP, 2)), (16, 6), (22, 5), (27, 5), (32, 5), (37, 5))
X_SENDS = ((0, 2), (2, 3), (5, 1))
AHEAD = 2
VMEM_LIMIT = 67043328 - 2 ** 21 - 2 ** 13
F32 = jnp.float32
BF16 = jnp.bfloat16


def iota(shape, dim):
    return lax.broadcasted_iota(jnp.int32, shape, dim)


def to_col(row):
    n = row.shape[1]
    return jnp.sum(jnp.where(iota((32, n), 0) == iota((32, n), 1), row, 0.0), axis=1, keepdims=True)


def pack_row(m, s, t):
    sub, lane = iota((32, 128), 0), iota((32, 128), 1)
    picked = jnp.where(lane == sub, m, jnp.where(lane == sub + 32, s, jnp.where(lane == sub + 64, t, 0.0)))
    return jnp.sum(picked, axis=0, keepdims=True)


def kernel(tok, h_hbm, w_hbm, temp_hbm, tgt_hbm, out_ref, tgt_out_ref,
           h_buf, temp_buf, tgt_buf, w_buf, part, far_in, side_in, near_in, x_part, x_src, x_in, piece_m, piece_s, piece_t,
           msg_src, msg_in, stats, res_src, res_in,
           h_sem, temp_sem, tgt_sem, w_sem, sub_w, sub_send, sub_recv, out_send, far_send, far_recv, side_recv, near_send, near_recv, xp_send, xp_recv, x_send, x_recv,
           msg_send, msg_recv, st_send, st_recv, res_send, res_recv, ready):
    z, v = lax.axis_index("hid"), lax.axis_index("vocab")
    outer = (z == 0) | (z == 3)
    inner = (z == 1) | (z == 2)
    far = jnp.where(z < 2, z + 1, z - 1)
    near = jnp.where(z == 1, 0, 3)
    cols = NP * tok
    last = 3 * NP - NX

    def w_load(rel, i, lane):
        slot = lax.rem(i, AHEAD) * 4 + lane
        owner = jnp.where(z < 2, rel, 3 - rel)
        start = pl.multiple_of(owner * cols + i * tok, tok)
        return pltpu.make_async_copy(w_hbm.at[:, pl.ds(start, tok)], w_buf.at[slot], w_sem.at[slot])

    h_copy = pltpu.make_async_copy(h_hbm, h_buf, h_sem)
    temp_copy = pltpu.make_async_copy(temp_hbm, temp_buf, temp_sem)
    tgt_copy = pltpu.make_async_copy(tgt_hbm, tgt_buf, tgt_sem)
    barrier = pltpu.get_barrier_semaphore()

    def greet(dev):
        pl.semaphore_signal(barrier, inc=1, device_id=dev, device_id_type=MESH)

    def part_of(k):
        at = (0, tok // 8, tok // 2, tok)
        return pl.ds(at[k], at[k + 1] - at[k])

    def sub_load(k):
        owner = jnp.where(z < 2, 3, 0)
        at = part_of(k)
        start = pl.multiple_of(owner * cols + at.start, tok // 8)
        return pltpu.make_async_copy(w_hbm.at[:, pl.ds(start, at.size)], w_buf.at[0, :, at], sub_w.at[k])

    @pl.when(inner)
    def _():
        greet({"hid": near})

    h_copy.start()
    for k in range(SUB):
        sub_load(k).start()
    greet({"hid": far})

    @pl.when(inner)
    def _():
        for dv in range(1, 4):
            greet({"vocab": lax.rem(v + dv, 4)})

    temp_copy.start()
    tgt_copy.start()

    def product(rel, i, lane):
        w_load(rel, i, lane).wait()
        part[rel * NP + i] = jnp.dot(h_buf[...], w_buf[lax.rem(i, AHEAD) * 4 + lane], preferred_element_type=F32)

        @pl.when(i + AHEAD < NP)
        def _():
            w_load(rel, i + AHEAD, lane).start()

    def products(i):
        product(0, i, 1)
        product(2, i, 2)
        product(1, i, 3)

        @pl.when(i + 2 < NP)
        def _():
            product(3, i + 2, 0)

    def sub_product(k):
        sub_load(k).wait()
        part[3 * NP, :, part_of(k)] = jnp.dot(h_buf[...], w_buf[0, :, part_of(k)], preferred_element_type=F32)

    def sub_copy(k):
        src, dst = part.at[3 * NP + 1], far_in.at[1]
        if k < SUB:
            src, dst = part.at[3 * NP, :, part_of(k)], far_in.at[0, :, part_of(k)]
        return pltpu.make_async_remote_copy(src_ref=src, dst_ref=dst,
                                            send_sem=sub_send.at[k], recv_sem=sub_recv.at[k],
                                            device_id={"hid": far}, device_id_type=MESH)

    tri = (iota((128, 128), 0) <= iota((128, 128), 1)).astype(BF16)
    piece_m[...] = jnp.zeros_like(piece_m)
    piece_s[...] = jnp.zeros_like(piece_s)
    piece_t[...] = jnp.zeros_like(piece_t)

    def put(ref, lane, value):
        ref[...] = jnp.where(iota((32, 128), 1) == lane, value, ref[...])

    def finish(total, first, lane, store):
        logits = total * temp
        m = jnp.max(logits, axis=1, keepdims=True)
        e = jnp.exp(logits - m)
        n_blk = tok // 128
        terms = []
        for b in range(n_blk):
            blk = e[:, b * 128:(b + 1) * 128]
            hi = blk.astype(BF16)
            rest = blk - hi.astype(F32)
            mid = rest.astype(BF16)
            low = (rest - mid.astype(F32)).astype(BF16)
            terms += [hi, mid, low]
        sums = jnp.dot(jnp.concatenate(terms, axis=0), tri, preferred_element_type=F32)
        carry = jnp.zeros((32, 1), F32)
        hit = jnp.zeros((32, 128), F32)
        pos = tgt - first
        lanes = iota((32, 128), 1).astype(F32)
        for b in range(n_blk):
            s = sums[96 * b:96 * b + 96]
            c = (s[0:32] + s[32:64] + s[64:96]) + carry
            store(b, c)
            hit = hit + jnp.where(lanes == pos - float(b * 128), c, 0.0)
            carry = c[:, 127:128]
        put(piece_m, lane, m)
        put(piece_s, lane, carry)
        put(piece_t, lane, jnp.sum(hit, axis=1, keepdims=True))

    def first_token(owner, i):
        return (((v * 4 + owner) * NP + i) * tok).astype(F32)

    def scan_lanes(x):
        lane = iota((32, 128), 1)
        for shift in (1, 2, 4, 8):
            x = x + jnp.where(lane >= shift, pltpu.roll(x, shift, 1), 0.0)
        return x

    def combine(owner):
        lane = iota((32, 128), 1)
        live = lane < NP
        m_all, s_all, t_all = piece_m[...], piece_s[...], piece_t[...]
        m = jnp.max(jnp.where(live, m_all, m_all[:, 0:1]), axis=1, keepdims=True)
        scale = jnp.where(live, jnp.exp(jnp.where(live, m_all, m) - m), 0.0)
        tot = s_all * scale
        s = jnp.sum(tot, axis=1, keepdims=True)
        low = lane.astype(F32) * float(tok) + first_token(owner, 0)
        t = jnp.sum(jnp.where(low + float(tok) <= tgt, tot, jnp.where(low <= tgt, t_all * scale, 0.0)),
                    axis=1, keepdims=True)
        return pack_row(m, s, t)

    def far_copy(src, t, dst, sems):
        return pltpu.make_async_remote_copy(src_ref=src, dst_ref=dst.at[t], send_sem=far_send.at[lax.rem(t, RING)],
                                            recv_sem=sems.at[t], device_id={"hid": far}, device_id_type=MESH)

    def part_index(t):
        i, ph = lax.rem(t, NP), t // NP
        return (3 - ph) * NP + jnp.where(ph == 1, lax.rem(i + NP - NX, NP), i)

    def outer_copy(j):
        t, count = SENDS[j]
        return pltpu.make_async_remote_copy(src_ref=part.at[pl.ds(part_index(t), count)], dst_ref=far_in.at[pl.ds(t, count)],
                                            send_sem=out_send.at[j], recv_sem=far_recv.at[j],
                                            device_id={"hid": far}, device_id_type=MESH)

    def inner_copy(t):
        return far_copy(far_in.at[t], t, side_in, side_recv)

    def near_copy(g):
        return pltpu.make_async_remote_copy(src_ref=side_in.at[g], dst_ref=near_in.at[g],
                                            send_sem=near_send.at[lax.rem(g, RING)], recv_sem=near_recv.at[g],
                                            device_id={"hid": near}, device_id_type=MESH)

    def x_part_copy(k):
        return pltpu.make_async_remote_copy(src_ref=side_in.at[NP + k], dst_ref=x_part.at[k],
                                            send_sem=xp_send.at[k], recv_sem=xp_recv.at[k],
                                            device_id={"hid": near}, device_id_type=MESH)

    def x_copy(j):
        at = pl.ds(*X_SENDS[j])
        return pltpu.make_async_remote_copy(src_ref=x_src.at[at], dst_ref=x_in.at[at], send_sem=x_send.at[j],
                                            recv_sem=x_recv.at[j], device_id={"hid": far}, device_id_type=MESH)

    msg_copy = pltpu.make_async_remote_copy(src_ref=msg_src, dst_ref=msg_in, send_sem=msg_send, recv_sem=msg_recv,
                                            device_id={"hid": far}, device_id_type=MESH)

    @pl.when(inner)
    def _():
        for k in range(SUB):
            sub_copy(k).wait_recv()

    h_copy.wait()
    for k in range(SUB):
        sub_product(k)
        if k == 0:
            for i in range(AHEAD):
                for lane, rel in ((0, 3), (1, 0), (2, 2), (3, 1)):
                    j = 1 - i if lane == 0 else i
                    if j or lane:
                        w_load(rel, j, lane).start()

            @pl.when(outer)
            def _():
                pl.semaphore_wait(barrier, 1)

        @pl.when(outer)
        def _(k=k):
            sub_copy(k).start()

    w_load(3, AHEAD, 0).start()
    product(3, 1, 0)

    @pl.when(outer)
    def _():
        sub_copy(SUB).start()

    temp_copy.wait()
    tgt_copy.wait()
    temp = to_col(temp_buf[...])
    tgt = to_col(tgt_buf[...].astype(F32))

    @pl.when(inner)
    def _():
        pl.semaphore_wait(barrier, 5)
        pl.semaphore_signal(ready, inc=1, device_id={"hid": far}, device_id_type=MESH)

    def out_store(i):
        def store(b, c):
            out_ref[:, pl.ds(pl.multiple_of(i * tok + b * 128, 128), 128)] = c
        return store

    @pl.when(outer)
    def _():
        def step(t, _):
            i = lax.rem(t, NP)

            for j, (first, _) in enumerate(SENDS):
                @pl.when(t == first)
                def _(j=j):
                    if j >= RING:
                        outer_copy(j - RING).wait_send()
                    outer_copy(j).start()

            @pl.when(t == 0)
            def _():
                sub_copy(1).wait_send()

            @pl.when(t < NP)
            def _():
                products(i)

            @pl.when((t >= NP) & (t < 2 * NP))
            def _():
                near_copy(i).wait_recv()
                finish(part[i] + near_in[i], first_token(z, i), i, out_store(i))

            @pl.when((t >= XSTEP) & (t < XSTEP + NX))
            def _():
                k = t - XSTEP

                def store(b, c):
                    x_src[k, :, b * 128:(b + 1) * 128] = c
                x_part_copy(k).wait_recv()
                finish(part[2 * NP - NX + k] + x_part[k], first_token(far, NP - NX + k), NP + k, store)

            @pl.when(t == XSTEP + NX)
            def _():
                sub = iota((8, 128), 0)
                tile = jnp.where(sub == 0, combine(z), 0.0)
                for k in range(NX):
                    lane = NP + k
                    row = pack_row(piece_m[:, lane:lane + 1], piece_s[:, lane:lane + 1], piece_t[:, lane:lane + 1])
                    tile = jnp.where(sub == k + 1, row, tile)
                msg_src[...] = tile

            @pl.when(t == XSTEP + NX + 1)
            def _():
                msg_copy.start()

            return ()

        lax.fori_loop(0, last, step, ())
        for j in range(len(X_SENDS)):
            x_copy(j).start()
        for k in (0, *range(2, SUB + 1)):
            sub_copy(k).wait_send()
        for k in range(RING):
            outer_copy(len(SENDS) - RING + k).wait_send()
        msg_copy.wait_send()

    @pl.when(inner)
    def _():
        def step(t, _):
            i = lax.rem(t, NP)
            g = t - LAG

            @pl.when(t == 1)
            def _():
                sub_copy(SUB).wait_recv()

            for j, (first, _) in enumerate(SENDS):
                @pl.when(t == first)
                def _(j=j):
                    outer_copy(j).wait_recv()

            @pl.when((t >= 1) & (t <= 2 * NP))
            def _():
                @pl.when(t - 1 >= RING)
                def _():
                    inner_copy(t - 1 - RING).wait_send()
                inner_copy(t - 1).start()

            @pl.when((g >= 1) & (g <= NP))
            def _():
                @pl.when(g - 1 >= RING)
                def _():
                    near_copy(g - 1 - RING).wait_send()
                near_copy(g - 1).start()

            for k in range(NX):
                @pl.when(g - 1 == NP + k)
                def _(k=k):
                    x_part_copy(k).start()

            @pl.when(t < 2 * NP)
            def _():
                far_in[t] = far_in[t] + part[part_index(t)]

            @pl.when((g >= 0) & (g < 2 * NP))
            def _():
                far_copy(far_in.at[g], g, side_in, side_recv).wait_recv()

                @pl.when(g < NP + NX)
                def _():
                    side_in[g] = side_in[g] + part[jnp.where(g < NP, g, g + NP - NX)]

            @pl.when(t < NP)
            def _():
                products(i)

            @pl.when(t >= 2 * NP)
            def _():
                finish(part[NP + i] + side_in[NP + NX + i] + far_in[t], first_token(z, i), i, out_store(i))

            return ()

        lax.fori_loop(0, last, step, ())
        msg_copy.wait_recv()
        msg = msg_in[...]
        for k in range(NX):
            lane = NP - NX + k
            row = msg[k + 1:k + 2]
            put(piece_m, lane, to_col(row))
            put(piece_s, lane, to_col(pltpu.roll(row, 96, 1)))
            put(piece_t, lane, to_col(pltpu.roll(row, 64, 1)))
        mine = combine(z)
        theirs = msg[0:1]
        sub, lane = iota((8, 128), 0), iota((8, 128), 1)
        tile = jnp.where(sub == 0, jnp.where(z == 1, theirs, mine),
                         jnp.where(sub == 1, jnp.where(z == 1, mine, theirs), jnp.where(lane < 32, mine, 0.0)))
        stats[2 * v + z - 1] = tile

    slot = 2 * v + z - 1

    def st_copy(slot, cross, dv):
        return pltpu.make_async_remote_copy(src_ref=stats.at[slot], dst_ref=stats.at[slot],
                                            send_sem=st_send.at[4 * cross + dv], recv_sem=st_recv.at[slot],
                                            device_id={"hid": far if cross else z, "vocab": lax.rem(v + dv, 4)},
                                            device_id_type=MESH)

    peers = [(cross, dv) for cross in (1, 0) for dv in range(4) if cross or dv]
    res_copy = pltpu.make_async_remote_copy(src_ref=res_src, dst_ref=res_in, send_sem=res_send, recv_sem=res_recv,
                                            device_id={"hid": near}, device_id_type=MESH)

    def settle(m_row, s_row, below_row):
        m_col, s_col, below = to_col(m_row), to_col(s_row), to_col(below_row)
        alive = iota((32, 128), 1) < NP
        mult = jnp.exp(jnp.where(alive, piece_m[...], m_col) - m_col)
        totals = jnp.where(alive, piece_s[...] * mult, 0.0)
        return mult / s_col, (below + (scan_lanes(totals) - totals)) / s_col

    def spread(i, src, mult, shift):
        out_ref[:, i * tok:(i + 1) * tok] = src * mult[:, i:i + 1] + shift[:, i:i + 1]

    @pl.when(inner)
    def _():
        pl.semaphore_wait(ready, 1)
        for cross, dv in peers:
            st_copy(slot, cross, dv).start()
        for k in range(RING):
            inner_copy(2 * NP - RING + k).wait_send()
            near_copy(NP - RING + k).wait_send()
        for k in range(NX):
            x_part_copy(k).wait_send()
        for other in range(8):
            @pl.when(slot != other)
            def _(other=other):
                st_copy(other, 0, 1).wait_recv()

        table = stats[...].reshape(64, 128)
        row_id = iota((64, 128), 0)
        m_row = jnp.max(table, axis=0, keepdims=True)
        scale = jnp.exp(table - m_row)
        live = (row_id & 7) < 2
        tot = jnp.where(live, pltpu.roll(table, 96, 1) * scale, 0.0)
        t_val = jnp.where(live, pltpu.roll(table, 64, 1) * scale, 0.0)
        s_row = jnp.sum(tot, axis=0, keepdims=True)

        def below(zz):
            me = v * 16 + (zz // 2) * 8 + lax.rem(zz, 2)
            return jnp.sum(jnp.where(row_id < me, tot, 0.0), axis=0, keepdims=True)

        low = (((row_id >> 3) * 2 + (row_id & 7)) * cols).astype(F32)
        tgt_lanes = jnp.sum(jnp.where(iota((32, 128), 0) == iota((32, 128), 1), tgt, 0.0), axis=0, keepdims=True)
        at_tgt = jnp.sum(jnp.where(low + float(cols) <= tgt_lanes, tot, jnp.where(low <= tgt_lanes, t_val, 0.0)),
                         axis=0, keepdims=True) / s_row
        sub = iota((8, 128), 0)
        res_src[...] = jnp.where(sub == 0, m_row, jnp.where(sub == 1, s_row, jnp.where(sub == 2, below(near), at_tgt)))
        tgt_out_ref[...] = at_tgt[:, 0:32]
        mult, shift = settle(m_row, s_row, below(z))
        res_copy.start()
        for i in range(NP - NX):
            spread(i, out_ref[:, i * tok:(i + 1) * tok], mult, shift)
        for cross, dv in peers:
            st_copy(slot, cross, dv).wait_send()
        res_copy.wait_send()
        for j, (first, count) in enumerate(X_SENDS):
            x_copy(j).wait_recv()
            for k in range(first, first + count):
                spread(NP - NX + k, x_in[k], mult, shift)

    @pl.when(outer)
    def _():
        res_copy.wait_recv()
        res = res_in[...]
        tgt_out_ref[...] = res[3:4, 0:32]
        mult, shift = settle(res[0:1], res[1:2], res[2:3])
        for i in range(NP):
            spread(i, out_ref[:, i * tok:(i + 1) * tok], mult, shift)
        for j in range(len(X_SENDS)):
            x_copy(j).wait_send()


def write_kernel(table_ref, at_tgt_ref, table_hbm, at_tgt_hbm, sem, at_sem):
    copies = (pltpu.make_async_copy(table_ref, table_hbm, sem), pltpu.make_async_copy(at_tgt_ref, at_tgt_hbm, at_sem))
    for c in copies:
        c.start()
    for c in copies:
        c.wait()


def solution(mesh):
    assert mesh.shape["hid"] == 4 and mesh.shape["vocab"] == 4

    def local_step(h_blk, w_blk, temp_blk, tgt_blk):
        rows, depth = h_blk.shape
        cols = w_blk.shape[1] // 4
        tok = cols // NP
        assert rows == 32 and tok % 128 == 0
        block = (rows, tok)
        vmem, dma = pltpu.VMEM, pltpu.SemaphoreType.DMA
        hbm = pl.BlockSpec(memory_space=pltpu.MemorySpace.HBM)
        in_vmem = pl.BlockSpec(memory_space=pltpu.VMEM)
        shapes = (jax.ShapeDtypeStruct((rows, cols), F32), jax.ShapeDtypeStruct((1, rows), F32))
        table, at_tgt = pl.pallas_call(
            functools.partial(kernel, tok),
            out_shape=(pltpu.VMEM((rows, cols), F32), pltpu.VMEM((1, rows), F32)),
            in_specs=[hbm] * 4,
            out_specs=(in_vmem, in_vmem),
            scratch_shapes=[
                vmem((rows, depth), BF16), vmem((1, rows), F32), vmem((1, rows), jnp.int32),
                vmem((4 * AHEAD, depth, tok), BF16),
                vmem((4 * NP, *block), F32),
                vmem((3 * NP, *block), F32),
                vmem((2 * NP, *block), F32),
                vmem((NP, *block), F32),
                vmem((NX, *block), F32),
                vmem((NX, *block), F32),
                vmem((NX, *block), F32),
                vmem((32, 128), F32),
                vmem((32, 128), F32),
                vmem((32, 128), F32),
                vmem((8, 128), F32), vmem((8, 128), F32), vmem((8, 8, 128), F32),
                vmem((8, 128), F32), vmem((8, 128), F32),
                dma, dma, dma, dma((4 * AHEAD,)), dma((SUB,)), dma((SUB + 1,)), dma((SUB + 1,)), dma((len(SENDS),)),
                dma((RING,)), dma((len(SENDS),)), dma((2 * NP,)),
                dma((RING,)), dma((NP,)),
                dma((NX,)), dma((NX,)), dma((len(X_SENDS),)), dma((len(X_SENDS),)),
                dma, dma, dma((8,)), dma((8,)), dma, dma, pltpu.SemaphoreType.REGULAR,
            ],
            compiler_params=pltpu.CompilerParams(collective_id=0, has_side_effects=True, vmem_limit_bytes=VMEM_LIMIT),
            name="head_cdf",
        )(h_blk, w_blk, temp_blk.reshape(1, rows), tgt_blk.reshape(1, rows))
        table, at_tgt = pl.pallas_call(
            write_kernel,
            out_shape=shapes,
            in_specs=[in_vmem, in_vmem],
            out_specs=(hbm, hbm),
            scratch_shapes=[dma, dma],
            compiler_params=pltpu.CompilerParams(vmem_limit_bytes=2 ** 20),
            name="write",
        )(table, at_tgt)
        return table, at_tgt.reshape(rows)

    return jax.shard_map(local_step, mesh=mesh,
                         in_specs=(P("data", "hid"), P("hid", "vocab"), P("data"), P("data")),
                         out_specs=(P("data", ("vocab", "hid")), P("data")), check_vma=False)
```

```python
import functools

import jax
import jax.numpy as jnp
from jax import lax
from jax.experimental import pallas as pl
from jax.experimental.pallas import tpu as pltpu
from jax.sharding import PartitionSpec as P

MESH = pl.DeviceIdType.MESH
NP = 16
NX = 6
RING = 2
LAG = 4
XSTEP = 2 * NP - 3
SUB = 3
SENDS = (*((t, 2) for t in range(2, NP, 2)), (16, 6), (22, 5), (27, 5), (32, 5), (37, 5))
X_SENDS = ((0, 5), (5, 1))
AHEAD = 2
VMEM_LIMIT = 67043328 - 2 ** 21 - 2 ** 13
F32 = jnp.float32
BF16 = jnp.bfloat16


def iota(shape, dim):
    return lax.broadcasted_iota(jnp.int32, shape, dim)


def to_col(row):
    n = row.shape[1]
    return jnp.sum(jnp.where(iota((32, n), 0) == iota((32, n), 1), row, 0.0), axis=1, keepdims=True)


def pack_row(m, s, t):
    sub, lane = iota((32, 128), 0), iota((32, 128), 1)
    picked = jnp.where(lane == sub, m, jnp.where(lane == sub + 32, s, jnp.where(lane == sub + 64, t, 0.0)))
    return jnp.sum(picked, axis=0, keepdims=True)


def kernel(tok, h_hbm, w_hbm, temp_hbm, tgt_hbm, out_ref, tgt_out_ref,
           h_buf, temp_buf, tgt_buf, w_buf, part, far_in, side_in, near_in, x_part, x_src, x_in, piece_m, piece_s, piece_t,
           msg_src, msg_in, stats, res_src, res_in,
           h_sem, temp_sem, tgt_sem, w_sem, sub_w, sub_send, sub_recv, out_send, far_send, far_recv, side_recv, near_send, near_recv, xp_send, xp_recv, x_send, x_recv,
           msg_send, msg_recv, st_send, st_recv, res_send, res_recv, ready):
    z, v = lax.axis_index("hid"), lax.axis_index("vocab")
    outer = (z == 0) | (z == 3)
    inner = (z == 1) | (z == 2)
    far = jnp.where(z < 2, z + 1, z - 1)
    near = jnp.where(z == 1, 0, 3)
    cols = NP * tok
    last = 3 * NP - NX

    def w_load(rel, i, lane):
        slot = lax.rem(i, AHEAD) * 4 + lane
        owner = jnp.where(z < 2, rel, 3 - rel)
        start = pl.multiple_of(owner * cols + i * tok, tok)
        return pltpu.make_async_copy(w_hbm.at[:, pl.ds(start, tok)], w_buf.at[slot], w_sem.at[slot])

    h_copy = pltpu.make_async_copy(h_hbm, h_buf, h_sem)
    temp_copy = pltpu.make_async_copy(temp_hbm, temp_buf, temp_sem)
    tgt_copy = pltpu.make_async_copy(tgt_hbm, tgt_buf, tgt_sem)
    barrier = pltpu.get_barrier_semaphore()

    def greet(dev):
        pl.semaphore_signal(barrier, inc=1, device_id=dev, device_id_type=MESH)

    def part_of(k):
        at = (0, tok // 8, tok // 2, tok)
        return pl.ds(at[k], at[k + 1] - at[k])

    def sub_load(k):
        owner = jnp.where(z < 2, 3, 0)
        at = part_of(k)
        start = pl.multiple_of(owner * cols + at.start, tok // 8)
        return pltpu.make_async_copy(w_hbm.at[:, pl.ds(start, at.size)], w_buf.at[0, :, at], sub_w.at[k])

    @pl.when(inner)
    def _():
        greet({"hid": near})

    h_copy.start()
    for k in range(SUB):
        sub_load(k).start()
    greet({"hid": far})

    @pl.when(inner)
    def _():
        for dv in range(1, 4):
            greet({"vocab": lax.rem(v + dv, 4)})

    temp_copy.start()
    tgt_copy.start()

    def product(rel, i, lane):
        w_load(rel, i, lane).wait()
        part[rel * NP + i] = jnp.dot(h_buf[...], w_buf[lax.rem(i, AHEAD) * 4 + lane], preferred_element_type=F32)

        @pl.when(i + AHEAD < NP)
        def _():
            w_load(rel, i + AHEAD, lane).start()

    def products(i):
        product(0, i, 1)
        product(2, i, 2)
        product(1, i, 3)

        @pl.when(i + 2 < NP)
        def _():
            product(3, i + 2, 0)

    def sub_product(k):
        sub_load(k).wait()
        part[3 * NP, :, part_of(k)] = jnp.dot(h_buf[...], w_buf[0, :, part_of(k)], preferred_element_type=F32)

    def sub_copy(k):
        src, dst = part.at[3 * NP + 1], far_in.at[1]
        if k < SUB:
            src, dst = part.at[3 * NP, :, part_of(k)], far_in.at[0, :, part_of(k)]
        return pltpu.make_async_remote_copy(src_ref=src, dst_ref=dst,
                                            send_sem=sub_send.at[k], recv_sem=sub_recv.at[k],
                                            device_id={"hid": far}, device_id_type=MESH)

    tri = (iota((128, 128), 0) <= iota((128, 128), 1)).astype(BF16)
    piece_m[...] = jnp.zeros_like(piece_m)
    piece_s[...] = jnp.zeros_like(piece_s)
    piece_t[...] = jnp.zeros_like(piece_t)

    def put(ref, lane, value):
        ref[...] = jnp.where(iota((32, 128), 1) == lane, value, ref[...])

    def finish(total, first, lane, store):
        logits = total * temp
        m = jnp.max(logits, axis=1, keepdims=True)
        e = jnp.exp(logits - m)
        n_blk = tok // 128
        terms = []
        for b in range(n_blk):
            blk = e[:, b * 128:(b + 1) * 128]
            hi = blk.astype(BF16)
            rest = blk - hi.astype(F32)
            mid = rest.astype(BF16)
            low = (rest - mid.astype(F32)).astype(BF16)
            terms += [hi, mid, low]
        sums = jnp.dot(jnp.concatenate(terms, axis=0), tri, preferred_element_type=F32)
        carry = jnp.zeros((32, 1), F32)
        hit = jnp.zeros((32, 128), F32)
        pos = tgt - first
        lanes = iota((32, 128), 1).astype(F32)
        for b in range(n_blk):
            s = sums[96 * b:96 * b + 96]
            c = (s[0:32] + s[32:64] + s[64:96]) + carry
            store(b, c)
            hit = hit + jnp.where(lanes == pos - float(b * 128), c, 0.0)
            carry = c[:, 127:128]
        put(piece_m, lane, m)
        put(piece_s, lane, carry)
        put(piece_t, lane, jnp.sum(hit, axis=1, keepdims=True))

    def first_token(owner, i):
        return (((v * 4 + owner) * NP + i) * tok).astype(F32)

    def scan_lanes(x):
        lane = iota((32, 128), 1)
        for shift in (1, 2, 4, 8):
            x = x + jnp.where(lane >= shift, pltpu.roll(x, shift, 1), 0.0)
        return x

    def combine(owner):
        lane = iota((32, 128), 1)
        live = lane < NP
        m_all, s_all, t_all = piece_m[...], piece_s[...], piece_t[...]
        m = jnp.max(jnp.where(live, m_all, m_all[:, 0:1]), axis=1, keepdims=True)
        scale = jnp.where(live, jnp.exp(jnp.where(live, m_all, m) - m), 0.0)
        tot = s_all * scale
        s = jnp.sum(tot, axis=1, keepdims=True)
        low = lane.astype(F32) * float(tok) + first_token(owner, 0)
        t = jnp.sum(jnp.where(low + float(tok) <= tgt, tot, jnp.where(low <= tgt, t_all * scale, 0.0)),
                    axis=1, keepdims=True)
        return pack_row(m, s, t)

    def far_copy(src, t, dst, sems):
        return pltpu.make_async_remote_copy(src_ref=src, dst_ref=dst.at[t], send_sem=far_send.at[lax.rem(t, RING)],
                                            recv_sem=sems.at[t], device_id={"hid": far}, device_id_type=MESH)

    def part_index(t):
        i, ph = lax.rem(t, NP), t // NP
        return (3 - ph) * NP + jnp.where(ph == 1, lax.rem(i + NP - NX, NP), i)

    def outer_copy(j):
        t, count = SENDS[j]
        return pltpu.make_async_remote_copy(src_ref=part.at[pl.ds(part_index(t), count)], dst_ref=far_in.at[pl.ds(t, count)],
                                            send_sem=out_send.at[j], recv_sem=far_recv.at[j],
                                            device_id={"hid": far}, device_id_type=MESH)

    def inner_copy(t):
        return far_copy(far_in.at[t], t, side_in, side_recv)

    def near_copy(g):
        return pltpu.make_async_remote_copy(src_ref=side_in.at[g], dst_ref=near_in.at[g],
                                            send_sem=near_send.at[lax.rem(g, RING)], recv_sem=near_recv.at[g],
                                            device_id={"hid": near}, device_id_type=MESH)

    def x_part_copy(k):
        return pltpu.make_async_remote_copy(src_ref=side_in.at[NP + k], dst_ref=x_part.at[k],
                                            send_sem=xp_send.at[k], recv_sem=xp_recv.at[k],
                                            device_id={"hid": near}, device_id_type=MESH)

    def x_copy(j):
        at = pl.ds(*X_SENDS[j])
        return pltpu.make_async_remote_copy(src_ref=x_src.at[at], dst_ref=x_in.at[at], send_sem=x_send.at[j],
                                            recv_sem=x_recv.at[j], device_id={"hid": far}, device_id_type=MESH)

    msg_copy = pltpu.make_async_remote_copy(src_ref=msg_src, dst_ref=msg_in, send_sem=msg_send, recv_sem=msg_recv,
                                            device_id={"hid": far}, device_id_type=MESH)

    @pl.when(inner)
    def _():
        for k in range(SUB):
            sub_copy(k).wait_recv()

    h_copy.wait()
    for k in range(SUB):
        sub_product(k)
        if k == 0:
            for i in range(AHEAD):
                for lane, rel in ((0, 3), (1, 0), (2, 2), (3, 1)):
                    j = 1 - i if lane == 0 else i
                    if j or lane:
                        w_load(rel, j, lane).start()

            @pl.when(outer)
            def _():
                pl.semaphore_wait(barrier, 1)

        @pl.when(outer)
        def _(k=k):
            sub_copy(k).start()

    w_load(3, AHEAD, 0).start()
    product(3, 1, 0)

    @pl.when(outer)
    def _():
        sub_copy(SUB).start()

    temp_copy.wait()
    tgt_copy.wait()
    temp = to_col(temp_buf[...])
    tgt = to_col(tgt_buf[...].astype(F32))

    @pl.when(inner)
    def _():
        pl.semaphore_wait(barrier, 5)
        pl.semaphore_signal(ready, inc=1, device_id={"hid": far}, device_id_type=MESH)

    def out_store(i):
        def store(b, c):
            out_ref[:, pl.ds(pl.multiple_of(i * tok + b * 128, 128), 128)] = c
        return store

    @pl.when(outer)
    def _():
        def step(t, _):
            i = lax.rem(t, NP)

            for j, (first, _) in enumerate(SENDS):
                @pl.when(t == first)
                def _(j=j):
                    if j >= RING:
                        outer_copy(j - RING).wait_send()
                    outer_copy(j).start()

            @pl.when(t == 0)
            def _():
                sub_copy(1).wait_send()

            @pl.when(t < NP)
            def _():
                products(i)

            @pl.when((t >= NP) & (t < 2 * NP))
            def _():
                near_copy(i).wait_recv()
                finish(part[i] + near_in[i], first_token(z, i), i, out_store(i))

            @pl.when((t >= XSTEP) & (t < XSTEP + NX))
            def _():
                k = t - XSTEP

                def store(b, c):
                    x_src[k, :, b * 128:(b + 1) * 128] = c
                x_part_copy(k).wait_recv()
                finish(part[2 * NP - NX + k] + x_part[k], first_token(far, NP - NX + k), NP + k, store)

            @pl.when(t == XSTEP + NX)
            def _():
                sub = iota((8, 128), 0)
                tile = jnp.where(sub == 0, combine(z), 0.0)
                for k in range(NX):
                    lane = NP + k
                    row = pack_row(piece_m[:, lane:lane + 1], piece_s[:, lane:lane + 1], piece_t[:, lane:lane + 1])
                    tile = jnp.where(sub == k + 1, row, tile)
                msg_src[...] = tile

            @pl.when(t == XSTEP + NX + 1)
            def _():
                msg_copy.start()

            return ()

        lax.fori_loop(0, last, step, ())
        for j in range(len(X_SENDS)):
            x_copy(j).start()
        for k in (0, *range(2, SUB + 1)):
            sub_copy(k).wait_send()
        for k in range(RING):
            outer_copy(len(SENDS) - RING + k).wait_send()
        msg_copy.wait_send()

    @pl.when(inner)
    def _():
        def step(t, _):
            i = lax.rem(t, NP)
            g = t - LAG

            @pl.when(t == 1)
            def _():
                sub_copy(SUB).wait_recv()

            for j, (first, _) in enumerate(SENDS):
                @pl.when(t == first)
                def _(j=j):
                    outer_copy(j).wait_recv()

            @pl.when((t >= 1) & (t <= 2 * NP))
            def _():
                @pl.when(t - 1 >= RING)
                def _():
                    inner_copy(t - 1 - RING).wait_send()
                inner_copy(t - 1).start()

            @pl.when((g >= 1) & (g <= NP))
            def _():
                @pl.when(g - 1 >= RING)
                def _():
                    near_copy(g - 1 - RING).wait_send()
                near_copy(g - 1).start()

            for k in range(NX):
                @pl.when(g - 1 == NP + k)
                def _(k=k):
                    x_part_copy(k).start()

            @pl.when(t < 2 * NP)
            def _():
                far_in[t] = far_in[t] + part[part_index(t)]

            @pl.when((g >= 0) & (g < 2 * NP))
            def _():
                far_copy(far_in.at[g], g, side_in, side_recv).wait_recv()

                @pl.when(g < NP + NX)
                def _():
                    side_in[g] = side_in[g] + part[jnp.where(g < NP, g, g + NP - NX)]

            @pl.when(t < NP)
            def _():
                products(i)

            @pl.when(t >= 2 * NP)
            def _():
                finish(part[NP + i] + side_in[NP + NX + i] + far_in[t], first_token(z, i), i, out_store(i))

            return ()

        lax.fori_loop(0, last, step, ())
        msg_copy.wait_recv()
        msg = msg_in[...]
        for k in range(NX):
            lane = NP - NX + k
            row = msg[k + 1:k + 2]
            put(piece_m, lane, to_col(row))
            put(piece_s, lane, to_col(pltpu.roll(row, 96, 1)))
            put(piece_t, lane, to_col(pltpu.roll(row, 64, 1)))
        mine = combine(z)
        theirs = msg[0:1]
        sub, lane = iota((8, 128), 0), iota((8, 128), 1)
        tile = jnp.where(sub == 0, jnp.where(z == 1, theirs, mine),
                         jnp.where(sub == 1, jnp.where(z == 1, mine, theirs), jnp.where(lane < 32, mine, 0.0)))
        stats[2 * v + z - 1] = tile

    slot = 2 * v + z - 1

    def st_copy(slot, cross, dv):
        return pltpu.make_async_remote_copy(src_ref=stats.at[slot], dst_ref=stats.at[slot],
                                            send_sem=st_send.at[4 * cross + dv], recv_sem=st_recv.at[slot],
                                            device_id={"hid": far if cross else z, "vocab": lax.rem(v + dv, 4)},
                                            device_id_type=MESH)

    peers = [(cross, dv) for cross in (1, 0) for dv in range(4) if cross or dv]
    res_copy = pltpu.make_async_remote_copy(src_ref=res_src, dst_ref=res_in, send_sem=res_send, recv_sem=res_recv,
                                            device_id={"hid": near}, device_id_type=MESH)

    def settle(m_row, s_row, below_row):
        m_col, s_col, below = to_col(m_row), to_col(s_row), to_col(below_row)
        alive = iota((32, 128), 1) < NP
        mult = jnp.exp(jnp.where(alive, piece_m[...], m_col) - m_col)
        totals = jnp.where(alive, piece_s[...] * mult, 0.0)
        return mult / s_col, (below + (scan_lanes(totals) - totals)) / s_col

    def spread(i, src, mult, shift):
        out_ref[:, i * tok:(i + 1) * tok] = src * mult[:, i:i + 1] + shift[:, i:i + 1]

    @pl.when(inner)
    def _():
        pl.semaphore_wait(ready, 1)
        for cross, dv in peers:
            st_copy(slot, cross, dv).start()
        for k in range(RING):
            inner_copy(2 * NP - RING + k).wait_send()
            near_copy(NP - RING + k).wait_send()
        for k in range(NX):
            x_part_copy(k).wait_send()
        for other in range(8):
            @pl.when(slot != other)
            def _(other=other):
                st_copy(other, 0, 1).wait_recv()

        table = stats[...].reshape(64, 128)
        row_id = iota((64, 128), 0)
        m_row = jnp.max(table, axis=0, keepdims=True)
        scale = jnp.exp(table - m_row)
        live = (row_id & 7) < 2
        tot = jnp.where(live, pltpu.roll(table, 96, 1) * scale, 0.0)
        t_val = jnp.where(live, pltpu.roll(table, 64, 1) * scale, 0.0)
        s_row = jnp.sum(tot, axis=0, keepdims=True)

        def below(zz):
            me = v * 16 + (zz // 2) * 8 + lax.rem(zz, 2)
            return jnp.sum(jnp.where(row_id < me, tot, 0.0), axis=0, keepdims=True)

        low = (((row_id >> 3) * 2 + (row_id & 7)) * cols).astype(F32)
        tgt_lanes = jnp.sum(jnp.where(iota((32, 128), 0) == iota((32, 128), 1), tgt, 0.0), axis=0, keepdims=True)
        at_tgt = jnp.sum(jnp.where(low + float(cols) <= tgt_lanes, tot, jnp.where(low <= tgt_lanes, t_val, 0.0)),
                         axis=0, keepdims=True) / s_row
        sub = iota((8, 128), 0)
        res_src[...] = jnp.where(sub == 0, m_row, jnp.where(sub == 1, s_row, jnp.where(sub == 2, below(near), at_tgt)))
        tgt_out_ref[...] = at_tgt[:, 0:32]
        mult, shift = settle(m_row, s_row, below(z))
        res_copy.start()
        for i in range(NP - NX):
            spread(i, out_ref[:, i * tok:(i + 1) * tok], mult, shift)
        for cross, dv in peers:
            st_copy(slot, cross, dv).wait_send()
        res_copy.wait_send()
        for j, (first, count) in enumerate(X_SENDS):
            x_copy(j).wait_recv()
            for k in range(first, first + count):
                spread(NP - NX + k, x_in[k], mult, shift)

    @pl.when(outer)
    def _():
        res_copy.wait_recv()
        res = res_in[...]
        tgt_out_ref[...] = res[3:4, 0:32]
        mult, shift = settle(res[0:1], res[1:2], res[2:3])
        for i in range(NP):
            spread(i, out_ref[:, i * tok:(i + 1) * tok], mult, shift)
        for j in range(len(X_SENDS)):
            x_copy(j).wait_send()


def write_kernel(table_ref, at_tgt_ref, table_hbm, at_tgt_hbm, sem, at_sem):
    copies = (pltpu.make_async_copy(table_ref, table_hbm, sem), pltpu.make_async_copy(at_tgt_ref, at_tgt_hbm, at_sem))
    for c in copies:
        c.start()
    for c in copies:
        c.wait()


def solution(mesh):
    assert mesh.shape["hid"] == 4 and mesh.shape["vocab"] == 4

    def local_step(h_blk, w_blk, temp_blk, tgt_blk):
        rows, depth = h_blk.shape
        cols = w_blk.shape[1] // 4
        tok = cols // NP
        assert rows == 32 and tok % 128 == 0
        block = (rows, tok)
        vmem, dma = pltpu.VMEM, pltpu.SemaphoreType.DMA
        hbm = pl.BlockSpec(memory_space=pltpu.MemorySpace.HBM)
        in_vmem = pl.BlockSpec(memory_space=pltpu.VMEM)
        shapes = (jax.ShapeDtypeStruct((rows, cols), F32), jax.ShapeDtypeStruct((1, rows), F32))
        table, at_tgt = pl.pallas_call(
            functools.partial(kernel, tok),
            out_shape=(pltpu.VMEM((rows, cols), F32), pltpu.VMEM((1, rows), F32)),
            in_specs=[hbm] * 4,
            out_specs=(in_vmem, in_vmem),
            scratch_shapes=[
                vmem((rows, depth), BF16), vmem((1, rows), F32), vmem((1, rows), jnp.int32),
                vmem((4 * AHEAD, depth, tok), BF16),
                vmem((4 * NP, *block), F32),
                vmem((3 * NP, *block), F32),
                vmem((2 * NP, *block), F32),
                vmem((NP, *block), F32),
                vmem((NX, *block), F32),
                vmem((NX, *block), F32),
                vmem((NX, *block), F32),
                vmem((32, 128), F32),
                vmem((32, 128), F32),
                vmem((32, 128), F32),
                vmem((8, 128), F32), vmem((8, 128), F32), vmem((8, 8, 128), F32),
                vmem((8, 128), F32), vmem((8, 128), F32),
                dma, dma, dma, dma((4 * AHEAD,)), dma((SUB,)), dma((SUB + 1,)), dma((SUB + 1,)), dma((len(SENDS),)),
                dma((RING,)), dma((len(SENDS),)), dma((2 * NP,)),
                dma((RING,)), dma((NP,)),
                dma((NX,)), dma((NX,)), dma((len(X_SENDS),)), dma((len(X_SENDS),)),
                dma, dma, dma((8,)), dma((8,)), dma, dma, pltpu.SemaphoreType.REGULAR,
            ],
            compiler_params=pltpu.CompilerParams(collective_id=0, has_side_effects=True, vmem_limit_bytes=VMEM_LIMIT),
            name="head_cdf",
        )(h_blk, w_blk, temp_blk.reshape(1, rows), tgt_blk.reshape(1, rows))
        table, at_tgt = pl.pallas_call(
            write_kernel,
            out_shape=shapes,
            in_specs=[in_vmem, in_vmem],
            out_specs=(hbm, hbm),
            scratch_shapes=[dma, dma],
            compiler_params=pltpu.CompilerParams(vmem_limit_bytes=2 ** 20),
            name="write",
        )(table, at_tgt)
        return table, at_tgt.reshape(rows)

    return jax.shard_map(local_step, mesh=mesh,
                         in_specs=(P("data", "hid"), P("hid", "vocab"), P("data"), P("data")),
                         out_specs=(P("data", ("vocab", "hid")), P("data")), check_vma=False)
```

```python
import functools

import jax
import jax.numpy as jnp
from jax import lax
from jax.experimental import pallas as pl
from jax.experimental.pallas import tpu as pltpu
from jax.sharding import PartitionSpec as P

MESH = pl.DeviceIdType.MESH
NP = 16
NX = 6
RING = 2
LAG = 4
XSTEP = 2 * NP - 3
SUB = 3
SENDS = (*((t, 2) for t in range(2, NP, 2)), (16, 6), (22, 5), (27, 5), (32, 5), (37, 5))
X_SENDS = ((0, 5), (5, 1))
AHEAD = 2
VMEM_LIMIT = 67043328 - 2 ** 21 - 2 ** 13
F32 = jnp.float32
BF16 = jnp.bfloat16


def iota(shape, dim):
    return lax.broadcasted_iota(jnp.int32, shape, dim)


def to_col(row):
    n = row.shape[1]
    return jnp.sum(jnp.where(iota((32, n), 0) == iota((32, n), 1), row, 0.0), axis=1, keepdims=True)


def pack_row(m, s, t):
    sub, lane = iota((32, 128), 0), iota((32, 128), 1)
    picked = jnp.where(lane == sub, m, jnp.where(lane == sub + 32, s, jnp.where(lane == sub + 64, t, 0.0)))
    return jnp.sum(picked, axis=0, keepdims=True)


def kernel(tok, h_hbm, w_hbm, temp_hbm, tgt_hbm, out_ref, tgt_out_ref,
           h_buf, temp_buf, tgt_buf, w_buf, part, far_in, side_in, near_in, x_part, x_src, x_in, piece_m, piece_s, piece_t,
           msg_src, msg_in, stats, res_src, res_in,
           h_sem, temp_sem, tgt_sem, w_sem, sub_w, sub_send, sub_recv, out_send, far_send, far_recv, side_recv, near_send, near_recv, xp_send, xp_recv, x_send, x_recv,
           msg_send, msg_recv, st_send, st_recv, res_send, res_recv, ready):
    z, v = lax.axis_index("hid"), lax.axis_index("vocab")
    outer = (z == 0) | (z == 3)
    inner = (z == 1) | (z == 2)
    far = jnp.where(z < 2, z + 1, z - 1)
    near = jnp.where(z == 1, 0, 3)
    cols = NP * tok
    last = 3 * NP - NX

    def w_load(rel, i, lane):
        slot = lax.rem(i, AHEAD) * 4 + lane
        owner = jnp.where(z < 2, rel, 3 - rel)
        start = pl.multiple_of(owner * cols + i * tok, tok)
        return pltpu.make_async_copy(w_hbm.at[:, pl.ds(start, tok)], w_buf.at[slot], w_sem.at[slot])

    h_copy = pltpu.make_async_copy(h_hbm, h_buf, h_sem)
    temp_copy = pltpu.make_async_copy(temp_hbm, temp_buf, temp_sem)
    tgt_copy = pltpu.make_async_copy(tgt_hbm, tgt_buf, tgt_sem)
    barrier = pltpu.get_barrier_semaphore()

    def greet(dev):
        pl.semaphore_signal(barrier, inc=1, device_id=dev, device_id_type=MESH)

    def part_of(k):
        at = (0, tok // 8, 3 * tok // 8, tok)
        return pl.ds(at[k], at[k + 1] - at[k])

    def sub_load(k):
        owner = jnp.where(z < 2, 3, 0)
        at = part_of(k)
        start = pl.multiple_of(owner * cols + at.start, tok // 8)
        return pltpu.make_async_copy(w_hbm.at[:, pl.ds(start, at.size)], w_buf.at[0, :, at], sub_w.at[k])

    @pl.when(inner)
    def _():
        greet({"hid": near})

    h_copy.start()
    for k in range(SUB):
        sub_load(k).start()
    greet({"hid": far})

    @pl.when(inner)
    def _():
        for dv in range(1, 4):
            greet({"vocab": lax.rem(v + dv, 4)})

    temp_copy.start()
    tgt_copy.start()

    def product(rel, i, lane):
        w_load(rel, i, lane).wait()
        part[rel * NP + i] = jnp.dot(h_buf[...], w_buf[lax.rem(i, AHEAD) * 4 + lane], preferred_element_type=F32)

        @pl.when(i + AHEAD < NP)
        def _():
            w_load(rel, i + AHEAD, lane).start()

    def products(i):
        product(0, i, 1)
        product(2, i, 2)
        product(1, i, 3)

        @pl.when(i + 2 < NP)
        def _():
            product(3, i + 2, 0)

    def sub_product(k):
        sub_load(k).wait()
        part[3 * NP, :, part_of(k)] = jnp.dot(h_buf[...], w_buf[0, :, part_of(k)], preferred_element_type=F32)

    def sub_copy(k):
        src, dst = part.at[3 * NP + 1], far_in.at[1]
        if k < SUB:
            src, dst = part.at[3 * NP, :, part_of(k)], far_in.at[0, :, part_of(k)]
        return pltpu.make_async_remote_copy(src_ref=src, dst_ref=dst,
                                            send_sem=sub_send.at[k], recv_sem=sub_recv.at[k],
                                            device_id={"hid": far}, device_id_type=MESH)

    tri = (iota((128, 128), 0) <= iota((128, 128), 1)).astype(BF16)
    piece_m[...] = jnp.zeros_like(piece_m)
    piece_s[...] = jnp.zeros_like(piece_s)
    piece_t[...] = jnp.zeros_like(piece_t)

    def put(ref, lane, value):
        ref[...] = jnp.where(iota((32, 128), 1) == lane, value, ref[...])

    def finish(total, first, lane, store):
        logits = total * temp
        m = jnp.max(logits, axis=1, keepdims=True)
        e = jnp.exp(logits - m)
        n_blk = tok // 128
        terms = []
        for b in range(n_blk):
            blk = e[:, b * 128:(b + 1) * 128]
            hi = blk.astype(BF16)
            rest = blk - hi.astype(F32)
            mid = rest.astype(BF16)
            low = (rest - mid.astype(F32)).astype(BF16)
            terms += [hi, mid, low]
        sums = jnp.dot(jnp.concatenate(terms, axis=0), tri, preferred_element_type=F32)
        carry = jnp.zeros((32, 1), F32)
        hit = jnp.zeros((32, 128), F32)
        pos = tgt - first
        lanes = iota((32, 128), 1).astype(F32)
        for b in range(n_blk):
            s = sums[96 * b:96 * b + 96]
            c = (s[0:32] + s[32:64] + s[64:96]) + carry
            store(b, c)
            hit = hit + jnp.where(lanes == pos - float(b * 128), c, 0.0)
            carry = c[:, 127:128]
        put(piece_m, lane, m)
        put(piece_s, lane, carry)
        put(piece_t, lane, jnp.sum(hit, axis=1, keepdims=True))

    def first_token(owner, i):
        return (((v * 4 + owner) * NP + i) * tok).astype(F32)

    def scan_lanes(x):
        lane = iota((32, 128), 1)
        for shift in (1, 2, 4, 8):
            x = x + jnp.where(lane >= shift, pltpu.roll(x, shift, 1), 0.0)
        return x

    def combine(owner):
        lane = iota((32, 128), 1)
        live = lane < NP
        m_all, s_all, t_all = piece_m[...], piece_s[...], piece_t[...]
        m = jnp.max(jnp.where(live, m_all, m_all[:, 0:1]), axis=1, keepdims=True)
        scale = jnp.where(live, jnp.exp(jnp.where(live, m_all, m) - m), 0.0)
        tot = s_all * scale
        s = jnp.sum(tot, axis=1, keepdims=True)
        low = lane.astype(F32) * float(tok) + first_token(owner, 0)
        t = jnp.sum(jnp.where(low + float(tok) <= tgt, tot, jnp.where(low <= tgt, t_all * scale, 0.0)),
                    axis=1, keepdims=True)
        return pack_row(m, s, t)

    def far_copy(src, t, dst, sems):
        return pltpu.make_async_remote_copy(src_ref=src, dst_ref=dst.at[t], send_sem=far_send.at[lax.rem(t, RING)],
                                            recv_sem=sems.at[t], device_id={"hid": far}, device_id_type=MESH)

    def part_index(t):
        i, ph = lax.rem(t, NP), t // NP
        return (3 - ph) * NP + jnp.where(ph == 1, lax.rem(i + NP - NX, NP), i)

    def outer_copy(j):
        t, count = SENDS[j]
        return pltpu.make_async_remote_copy(src_ref=part.at[pl.ds(part_index(t), count)], dst_ref=far_in.at[pl.ds(t, count)],
                                            send_sem=out_send.at[j], recv_sem=far_recv.at[j],
                                            device_id={"hid": far}, device_id_type=MESH)

    def inner_copy(t):
        return far_copy(far_in.at[t], t, side_in, side_recv)

    def near_copy(g):
        return pltpu.make_async_remote_copy(src_ref=side_in.at[g], dst_ref=near_in.at[g],
                                            send_sem=near_send.at[lax.rem(g, RING)], recv_sem=near_recv.at[g],
                                            device_id={"hid": near}, device_id_type=MESH)

    def x_part_copy(k):
        return pltpu.make_async_remote_copy(src_ref=side_in.at[NP + k], dst_ref=x_part.at[k],
                                            send_sem=xp_send.at[k], recv_sem=xp_recv.at[k],
                                            device_id={"hid": near}, device_id_type=MESH)

    def x_copy(j):
        at = pl.ds(*X_SENDS[j])
        return pltpu.make_async_remote_copy(src_ref=x_src.at[at], dst_ref=x_in.at[at], send_sem=x_send.at[j],
                                            recv_sem=x_recv.at[j], device_id={"hid": far}, device_id_type=MESH)

    msg_copy = pltpu.make_async_remote_copy(src_ref=msg_src, dst_ref=msg_in, send_sem=msg_send, recv_sem=msg_recv,
                                            device_id={"hid": far}, device_id_type=MESH)

    @pl.when(inner)
    def _():
        for k in range(SUB):
            sub_copy(k).wait_recv()

    h_copy.wait()
    for k in range(SUB):
        sub_product(k)
        if k == 0:
            for i in range(AHEAD):
                for lane, rel in ((0, 3), (1, 0), (2, 2), (3, 1)):
                    j = 1 - i if lane == 0 else i
                    if j or lane:
                        w_load(rel, j, lane).start()

            @pl.when(outer)
            def _():
                pl.semaphore_wait(barrier, 1)

        @pl.when(outer)
        def _(k=k):
            sub_copy(k).start()

    w_load(3, AHEAD, 0).start()
    product(3, 1, 0)

    @pl.when(outer)
    def _():
        sub_copy(SUB).start()

    temp_copy.wait()
    tgt_copy.wait()
    temp = to_col(temp_buf[...])
    tgt = to_col(tgt_buf[...].astype(F32))

    @pl.when(inner)
    def _():
        pl.semaphore_wait(barrier, 5)
        pl.semaphore_signal(ready, inc=1, device_id={"hid": far}, device_id_type=MESH)

    def out_store(i):
        def store(b, c):
            out_ref[:, pl.ds(pl.multiple_of(i * tok + b * 128, 128), 128)] = c
        return store

    @pl.when(outer)
    def _():
        def step(t, _):
            i = lax.rem(t, NP)

            for j, (first, _) in enumerate(SENDS):
                @pl.when(t == first)
                def _(j=j):
                    if j >= RING:
                        outer_copy(j - RING).wait_send()
                    outer_copy(j).start()

            @pl.when(t == 0)
            def _():
                sub_copy(1).wait_send()

            @pl.when(t < NP)
            def _():
                products(i)

            @pl.when((t >= NP) & (t < 2 * NP))
            def _():
                near_copy(i).wait_recv()
                finish(part[i] + near_in[i], first_token(z, i), i, out_store(i))

            @pl.when((t >= XSTEP) & (t < XSTEP + NX))
            def _():
                k = t - XSTEP

                def store(b, c):
                    x_src[k, :, b * 128:(b + 1) * 128] = c
                x_part_copy(k).wait_recv()
                finish(part[2 * NP - NX + k] + x_part[k], first_token(far, NP - NX + k), NP + k, store)

            @pl.when(t == XSTEP + NX)
            def _():
                sub = iota((8, 128), 0)
                tile = jnp.where(sub == 0, combine(z), 0.0)
                for k in range(NX):
                    lane = NP + k
                    row = pack_row(piece_m[:, lane:lane + 1], piece_s[:, lane:lane + 1], piece_t[:, lane:lane + 1])
                    tile = jnp.where(sub == k + 1, row, tile)
                msg_src[...] = tile

            @pl.when(t == XSTEP + NX + 1)
            def _():
                msg_copy.start()

            return ()

        lax.fori_loop(0, last, step, ())
        for j in range(len(X_SENDS)):
            x_copy(j).start()
        for k in (0, *range(2, SUB + 1)):
            sub_copy(k).wait_send()
        for k in range(RING):
            outer_copy(len(SENDS) - RING + k).wait_send()
        msg_copy.wait_send()

    @pl.when(inner)
    def _():
        def step(t, _):
            i = lax.rem(t, NP)
            g = t - LAG

            @pl.when(t == 1)
            def _():
                sub_copy(SUB).wait_recv()

            for j, (first, _) in enumerate(SENDS):
                @pl.when(t == first)
                def _(j=j):
                    outer_copy(j).wait_recv()

            @pl.when((t >= 1) & (t <= 2 * NP))
            def _():
                @pl.when(t - 1 >= RING)
                def _():
                    inner_copy(t - 1 - RING).wait_send()
                inner_copy(t - 1).start()

            @pl.when((g >= 1) & (g <= NP))
            def _():
                @pl.when(g - 1 >= RING)
                def _():
                    near_copy(g - 1 - RING).wait_send()
                near_copy(g - 1).start()

            for k in range(NX):
                @pl.when(g - 1 == NP + k)
                def _(k=k):
                    x_part_copy(k).start()

            @pl.when(t < 2 * NP)
            def _():
                far_in[t] = far_in[t] + part[part_index(t)]

            @pl.when((g >= 0) & (g < 2 * NP))
            def _():
                far_copy(far_in.at[g], g, side_in, side_recv).wait_recv()

                @pl.when(g < NP + NX)
                def _():
                    side_in[g] = side_in[g] + part[jnp.where(g < NP, g, g + NP - NX)]

            @pl.when(t < NP)
            def _():
                products(i)

            @pl.when(t >= 2 * NP)
            def _():
                finish(part[NP + i] + side_in[NP + NX + i] + far_in[t], first_token(z, i), i, out_store(i))

            return ()

        lax.fori_loop(0, last, step, ())
        msg_copy.wait_recv()
        msg = msg_in[...]
        for k in range(NX):
            lane = NP - NX + k
            row = msg[k + 1:k + 2]
            put(piece_m, lane, to_col(row))
            put(piece_s, lane, to_col(pltpu.roll(row, 96, 1)))
            put(piece_t, lane, to_col(pltpu.roll(row, 64, 1)))
        mine = combine(z)
        theirs = msg[0:1]
        sub, lane = iota((8, 128), 0), iota((8, 128), 1)
        tile = jnp.where(sub == 0, jnp.where(z == 1, theirs, mine),
                         jnp.where(sub == 1, jnp.where(z == 1, mine, theirs), jnp.where(lane < 32, mine, 0.0)))
        stats[2 * v + z - 1] = tile

    slot = 2 * v + z - 1

    def st_copy(slot, cross, dv):
        return pltpu.make_async_remote_copy(src_ref=stats.at[slot], dst_ref=stats.at[slot],
                                            send_sem=st_send.at[4 * cross + dv], recv_sem=st_recv.at[slot],
                                            device_id={"hid": far if cross else z, "vocab": lax.rem(v + dv, 4)},
                                            device_id_type=MESH)

    peers = [(cross, dv) for cross in (1, 0) for dv in range(4) if cross or dv]
    res_copy = pltpu.make_async_remote_copy(src_ref=res_src, dst_ref=res_in, send_sem=res_send, recv_sem=res_recv,
                                            device_id={"hid": near}, device_id_type=MESH)

    def settle(m_row, s_row, below_row):
        m_col, s_col, below = to_col(m_row), to_col(s_row), to_col(below_row)
        alive = iota((32, 128), 1) < NP
        mult = jnp.exp(jnp.where(alive, piece_m[...], m_col) - m_col)
        totals = jnp.where(alive, piece_s[...] * mult, 0.0)
        return mult / s_col, (below + (scan_lanes(totals) - totals)) / s_col

    def spread(i, src, mult, shift):
        out_ref[:, i * tok:(i + 1) * tok] = src * mult[:, i:i + 1] + shift[:, i:i + 1]

    @pl.when(inner)
    def _():
        pl.semaphore_wait(ready, 1)
        for cross, dv in peers:
            st_copy(slot, cross, dv).start()
        for k in range(RING):
            inner_copy(2 * NP - RING + k).wait_send()
            near_copy(NP - RING + k).wait_send()
        for k in range(NX):
            x_part_copy(k).wait_send()
        for other in range(8):
            @pl.when(slot != other)
            def _(other=other):
                st_copy(other, 0, 1).wait_recv()

        table = stats[...].reshape(64, 128)
        row_id = iota((64, 128), 0)
        m_row = jnp.max(table, axis=0, keepdims=True)
        scale = jnp.exp(table - m_row)
        live = (row_id & 7) < 2
        tot = jnp.where(live, pltpu.roll(table, 96, 1) * scale, 0.0)
        t_val = jnp.where(live, pltpu.roll(table, 64, 1) * scale, 0.0)
        s_row = jnp.sum(tot, axis=0, keepdims=True)

        def below(zz):
            me = v * 16 + (zz // 2) * 8 + lax.rem(zz, 2)
            return jnp.sum(jnp.where(row_id < me, tot, 0.0), axis=0, keepdims=True)

        low = (((row_id >> 3) * 2 + (row_id & 7)) * cols).astype(F32)
        tgt_lanes = jnp.sum(jnp.where(iota((32, 128), 0) == iota((32, 128), 1), tgt, 0.0), axis=0, keepdims=True)
        at_tgt = jnp.sum(jnp.where(low + float(cols) <= tgt_lanes, tot, jnp.where(low <= tgt_lanes, t_val, 0.0)),
                         axis=0, keepdims=True) / s_row
        sub = iota((8, 128), 0)
        res_src[...] = jnp.where(sub == 0, m_row, jnp.where(sub == 1, s_row, jnp.where(sub == 2, below(near), at_tgt)))
        tgt_out_ref[...] = at_tgt[:, 0:32]
        mult, shift = settle(m_row, s_row, below(z))
        res_copy.start()
        for i in range(NP - NX):
            spread(i, out_ref[:, i * tok:(i + 1) * tok], mult, shift)
        for cross, dv in peers:
            st_copy(slot, cross, dv).wait_send()
        res_copy.wait_send()
        for j, (first, count) in enumerate(X_SENDS):
            x_copy(j).wait_recv()
            for k in range(first, first + count):
                spread(NP - NX + k, x_in[k], mult, shift)

    @pl.when(outer)
    def _():
        res_copy.wait_recv()
        res = res_in[...]
        tgt_out_ref[...] = res[3:4, 0:32]
        mult, shift = settle(res[0:1], res[1:2], res[2:3])
        for i in range(NP):
            spread(i, out_ref[:, i * tok:(i + 1) * tok], mult, shift)
        for j in range(len(X_SENDS)):
            x_copy(j).wait_send()


def write_kernel(table_ref, at_tgt_ref, table_hbm, at_tgt_hbm, sem, at_sem):
    copies = (pltpu.make_async_copy(table_ref, table_hbm, sem), pltpu.make_async_copy(at_tgt_ref, at_tgt_hbm, at_sem))
    for c in copies:
        c.start()
    for c in copies:
        c.wait()


def solution(mesh):
    assert mesh.shape["hid"] == 4 and mesh.shape["vocab"] == 4

    def local_step(h_blk, w_blk, temp_blk, tgt_blk):
        rows, depth = h_blk.shape
        cols = w_blk.shape[1] // 4
        tok = cols // NP
        assert rows == 32 and tok % 128 == 0
        block = (rows, tok)
        vmem, dma = pltpu.VMEM, pltpu.SemaphoreType.DMA
        hbm = pl.BlockSpec(memory_space=pltpu.MemorySpace.HBM)
        in_vmem = pl.BlockSpec(memory_space=pltpu.VMEM)
        shapes = (jax.ShapeDtypeStruct((rows, cols), F32), jax.ShapeDtypeStruct((1, rows), F32))
        table, at_tgt = pl.pallas_call(
            functools.partial(kernel, tok),
            out_shape=(pltpu.VMEM((rows, cols), F32), pltpu.VMEM((1, rows), F32)),
            in_specs=[hbm] * 4,
            out_specs=(in_vmem, in_vmem),
            scratch_shapes=[
                vmem((rows, depth), BF16), vmem((1, rows), F32), vmem((1, rows), jnp.int32),
                vmem((4 * AHEAD, depth, tok), BF16),
                vmem((4 * NP, *block), F32),
                vmem((3 * NP, *block), F32),
                vmem((2 * NP, *block), F32),
                vmem((NP, *block), F32),
                vmem((NX, *block), F32),
                vmem((NX, *block), F32),
                vmem((NX, *block), F32),
                vmem((32, 128), F32),
                vmem((32, 128), F32),
                vmem((32, 128), F32),
                vmem((8, 128), F32), vmem((8, 128), F32), vmem((8, 8, 128), F32),
                vmem((8, 128), F32), vmem((8, 128), F32),
                dma, dma, dma, dma((4 * AHEAD,)), dma((SUB,)), dma((SUB + 1,)), dma((SUB + 1,)), dma((len(SENDS),)),
                dma((RING,)), dma((len(SENDS),)), dma((2 * NP,)),
                dma((RING,)), dma((NP,)),
                dma((NX,)), dma((NX,)), dma((len(X_SENDS),)), dma((len(X_SENDS),)),
                dma, dma, dma((8,)), dma((8,)), dma, dma, pltpu.SemaphoreType.REGULAR,
            ],
            compiler_params=pltpu.CompilerParams(collective_id=0, has_side_effects=True, vmem_limit_bytes=VMEM_LIMIT),
            name="head_cdf",
        )(h_blk, w_blk, temp_blk.reshape(1, rows), tgt_blk.reshape(1, rows))
        table, at_tgt = pl.pallas_call(
            write_kernel,
            out_shape=shapes,
            in_specs=[in_vmem, in_vmem],
            out_specs=(hbm, hbm),
            scratch_shapes=[dma, dma],
            compiler_params=pltpu.CompilerParams(vmem_limit_bytes=2 ** 20),
            name="write",
        )(table, at_tgt)
        return table, at_tgt.reshape(rows)

    return jax.shard_map(local_step, mesh=mesh,
                         in_specs=(P("data", "hid"), P("hid", "vocab"), P("data"), P("data")),
                         out_specs=(P("data", ("vocab", "hid")), P("data")), check_vma=False)
```
